32 devices in a mesh: grp: 4 (over y, core), rows: 8 (over z, x).
Axes of the slice: x: 2, y: 2, z: 4, core: 2. Of those that a mesh axis runs over, the one named last changes fastest.
Arguments:
- rhs: float32 [2048, 64, 128], P(('grp', 'rows')), may hold values from -6 to 6
- fine_diag: bfloat16 [2048, 64, 64], P(('grp', 'rows')), may hold values from -0.2 to 1.2
- fine_smoother: bfloat16 [2048, 64, 64], P(('grp', 'rows')), may hold values from -4 to 4
- fine_blocks: bfloat16 [2048, 7, 64, 64], P(('grp', 'rows')), may hold values from -0.1796875 to 0.1796875
- fine_cols: int32 [2048, 7], P(('grp', 'rows')), may hold values from 0 to 2047, as said below
- aggregate: int32 [2048], P(('grp', 'rows')), may hold values from 0 to 511, as said below
- coarse_diag: bfloat16 [512, 64, 64], P('rows'), may hold values from -0.8 to 4.8
- coarse_smoother: bfloat16 [512, 64, 64], P('rows'), may hold values from -1 to 1
- coarse_blocks: bfloat16 [512, 7, 64, 64], P('rows'), may hold values from -0.71875 to 0.71875
- coarse_cols: int32 [512, 7], P('rows'), may hold values from 0 to 511, as said below
Outputs:
- solution: float32 [2048, 64, 128], P(('grp', 'rows'))
The draws below stay inside these ranges and needn't reach their ends.
Inputs may be any that keep to these rules, and one draw needn't show every extreme that they name: fine_cols row i names rows within 32 of i; the distance 32 is reached. coarse_cols row c names rows within 32 of c; the distance 32 is reached. `aggregate`: aggregate_i lies in [r * 64, (r + 1) * 64) with r = (i // 64) mod 8.
All inputs are finite; a program needn't handle non-finite values.
Results may differ from the reference program's by a relative error of at most 0.001.
The reference program's roundings to bfloat16 on the way count: a program that leaves them out, or rounds other values in their place, can miss the bound.
Values may be sent and summed in bfloat16 or wider, within the bound.
A program may use at most 128 MiB of HBM per device.

```python
import jax
import jax.numpy as jnp
from jax import lax

B = 64
NEIGH = 7
R_DEV = 64
NRHS = 128
C_DEV = 64
NF = 2048
NC = 512
N_ROWS = 8


def build_blocks(key, count, scale):
    shape = (count, B, B)
    noise = jnp.clip(0.04 * jax.random.normal(key, shape, jnp.float32), -0.16, 0.16)
    return scale * (jnp.eye(B, dtype=jnp.float32)[None] + noise)


def neighbour_columns(key, count, reach, block):
    key_distance, key_direction, key_chosen = jax.random.split(key, 3)
    distance = jax.random.randint(key_distance, (count, NEIGH), 1, reach + 1)
    direction = 2 * jax.random.randint(key_direction, (count, NEIGH), 0, 2) - 1
    offset = distance * direction
    row_ids = jnp.arange(count, dtype=jnp.int32)
    groups = count // block
    chosen = jax.random.randint(key_chosen, (groups, 2), 0, block)
    within = row_ids % block
    owner_block = row_ids // block
    low_hit = within == chosen[owner_block, 0]
    high_hit = within == chosen[owner_block, 1]
    first_slot = jnp.where(high_hit, reach, jnp.where(low_hit, -reach, offset[:, 0]))
    second_slot = jnp.where(row_ids == 0, -reach, jnp.where(row_ids == count - 1, reach, offset[:, 1]))
    offset = jnp.concatenate([first_slot[:, None], second_slot[:, None], offset[:, 2:]], axis=1)
    return jnp.clip(row_ids[:, None] + offset, 0, count - 1).astype(jnp.int32)


def draw_fine_diag(key, part):
    return build_blocks(jax.random.fold_in(key, 11), NF, 1.0).astype(jnp.bfloat16)


def draw_fine_smoother(key, part):
    return jnp.linalg.inv(build_blocks(jax.random.fold_in(key, 11), NF, 1.0)).astype(jnp.bfloat16)


def draw_coarse_diag(key, part):
    return build_blocks(jax.random.fold_in(key, 23), NC, 4.0).astype(jnp.bfloat16)


def draw_coarse_smoother(key, part):
    return jnp.linalg.inv(build_blocks(jax.random.fold_in(key, 23), NC, 4.0)).astype(jnp.bfloat16)


def draw_fine_cols(key, part):
    return neighbour_columns(jax.random.fold_in(key, 37), NF, R_DEV // 2, R_DEV)


def draw_coarse_cols(key, part):
    return neighbour_columns(jax.random.fold_in(key, 41), NC, C_DEV // 2, C_DEV)


def draw_aggregate(key, part):
    row_ids = jnp.arange(NF, dtype=jnp.int32)
    owner_row = row_ids // R_DEV % N_ROWS
    local_slot = jax.random.randint(jax.random.fold_in(key, 53), (NF,), 0, C_DEV)
    local_slot = jnp.where(row_ids == 0, 0, jnp.where(row_ids == NF - 1, C_DEV - 1, local_slot))
    return (owner_row * C_DEV + local_slot).astype(jnp.int32)


def shard_levels(key, extent, cuts, smallest, largest):
    def one(axis_at, parts):
        draws = jax.random.uniform(jax.random.fold_in(jax.random.fold_in(key, 6), axis_at), (parts,), jnp.float32, smallest / len(cuts), largest / len(cuts))
        return jnp.repeat(jnp.exp(draws), extent[axis_at] // parts).reshape((-1,) + (1,) * (len(extent) - axis_at - 1))

    gain = one(*cuts[0])
    for cut in cuts[1:]:
        gain = gain * one(*cut)
    return gain


def centred(key, shape, width, most, cuts=(), kind=jnp.bfloat16):
    entries = jax.random.normal(key, shape, jnp.float32) * width
    if len(cuts) > 0:
        entries = shard_levels(key, shape, cuts, -0.22, 0.18) * entries
    return jnp.clip(entries, min=-most, max=most).astype(kind)


def setup_inputs(seed: int = 0) -> dict:
    seeds = jax.random.split(jax.random.key(seed), 11)
    rhs = centred(seeds[0], (NF, B, NRHS), 1.0, 6.0, ((0, 32),), jnp.float32)
    fine_diag = draw_fine_diag(jax.random.fold_in(seeds[10], 71), 0)
    fine_smoother = draw_fine_smoother(jax.random.fold_in(seeds[10], 71), 0)
    fine_blocks = centred(seeds[3], (NF, NEIGH, B, B), 0.03, 0.1796875, ((0, 32),))
    fine_cols = draw_fine_cols(jax.random.fold_in(seeds[10], 71), 0)
    aggregate = draw_aggregate(jax.random.fold_in(seeds[10], 71), 0)
    coarse_diag = draw_coarse_diag(jax.random.fold_in(seeds[10], 71), 0)
    coarse_smoother = draw_coarse_smoother(jax.random.fold_in(seeds[10], 71), 0)
    coarse_blocks = centred(seeds[8], (NC, NEIGH, B, B), 0.12, 0.71875, ((0, 8),))
    coarse_cols = draw_coarse_cols(jax.random.fold_in(seeds[10], 71), 0)
    return dict(rhs=rhs, fine_diag=fine_diag, fine_smoother=fine_smoother, fine_blocks=fine_blocks, fine_cols=fine_cols, aggregate=aggregate, coarse_diag=coarse_diag, coarse_smoother=coarse_smoother, coarse_blocks=coarse_blocks, coarse_cols=coarse_cols)


damping = 0.8

def rounded(values):
    return lax.optimization_barrier(values.astype(jnp.bfloat16)).astype(jnp.float32)

def block_product(blocks, vector):
    return jnp.einsum('nab,nbk->nak', blocks.astype(jnp.float32), rounded(vector), precision=lax.Precision.HIGHEST)

def apply_operator(diag_blocks, off_blocks, columns, vector, height):
    vector_low = rounded(vector)
    group_count = vector.shape[0] // height

    def one_group(group_index):
        first_row = group_index * height
        diag_part = lax.dynamic_slice_in_dim(diag_blocks, first_row, height, 0).astype(jnp.float32)
        off_part = lax.dynamic_slice_in_dim(off_blocks, first_row, height, 0).astype(jnp.float32)
        column_part = lax.dynamic_slice_in_dim(columns, first_row, height, 0)
        own_rows = lax.dynamic_slice_in_dim(vector_low, first_row, height, 0)
        nearby = jnp.take(vector_low, column_part, axis=0)
        own_term = jnp.einsum('nab,nbk->nak', diag_part, own_rows, precision=lax.Precision.HIGHEST)
        off_term = jnp.einsum('njab,njbk->nak', off_part, nearby, precision=lax.Precision.HIGHEST)
        return own_term + off_term
    result = lax.map(one_group, jnp.arange(group_count, dtype=jnp.int32))
    return result.reshape(vector.shape)

def reference(rhs, fine_diag, fine_smoother, fine_blocks, fine_cols, aggregate, coarse_diag, coarse_smoother, coarse_blocks, coarse_cols):
    first_iterate = damping * block_product(fine_smoother, rhs)
    first_residual = rhs - apply_operator(fine_diag, fine_blocks, fine_cols, first_iterate, R_DEV)
    second_iterate = first_iterate + damping * block_product(fine_smoother, first_residual)
    second_residual = rhs - apply_operator(fine_diag, fine_blocks, fine_cols, second_iterate, R_DEV)
    coarse_rhs = jax.ops.segment_sum(second_residual, aggregate, num_segments=NC)
    coarse_first = damping * block_product(coarse_smoother, coarse_rhs)
    coarse_image = apply_operator(coarse_diag, coarse_blocks, coarse_cols, coarse_first, C_DEV)
    coarse_second = coarse_first + damping * block_product(coarse_smoother, coarse_rhs - coarse_image)
    return second_iterate + jnp.take(coarse_second, aggregate, axis=0)
```

```python
import functools

import jax
import jax.numpy as jnp
from jax import lax
from jax.experimental import pallas as pl
from jax.experimental.pallas import tpu as pltpu
from jax.sharding import PartitionSpec as P

MESH = pl.DeviceIdType.MESH
damping = 0.8
steps = 8
depth = 3
parts = 4
low = jnp.bfloat16
f32 = jnp.float32


def dot(a, b):
    return jnp.dot(a, b, preferred_element_type=f32)


def row_product(i, columns, at, base, offs, diag, extended, own):
    count = offs.shape[1]
    last = extended.shape[0] - 1
    vectors = [extended[jnp.clip(columns[k, at] - base, 0, last)] for k in range(count)] + [extended[own]]
    blocks = [offs[i, k] for k in range(count)] + [diag[i]]
    total = None
    for p in range(0, count + 1, 4):
        term = dot(
            jnp.concatenate(blocks[p : p + 4], axis=1),
            jnp.concatenate(vectors[p : p + 4], axis=0),
        )
        total = term if total is None else total + term
    return total


def kernel(
    groups, ranks,
    fine_cols, coarse_cols, aggregate,
    rhs_hbm, diag_hbm, smoother_hbm, blocks_hbm, cdiag_hbm, csmoother_hbm, cblocks_hbm,
    iterate_hbm, correction_hbm,
    rhs, diag, smoother, blocks, cdiag, csmoother, cblocks,
    ext1, ext2, landing1, landing2, iterate, sums, partial, from_partner, chip_send, chip_recv, crhs, cfirst, cext, correction, chain,
    load_sem, out_sem, halo_send, halo_recv, rs_send, rs_recv, rc_send, rc_recv,
    piece_send, piece_recv, ag_send, ag_recv, fwd_send, fwd_recv,
):
    g = lax.axis_index("grp")
    r = lax.axis_index("rows")
    height = rhs.shape[0]
    margin = height // 2
    cheight = partial.shape[0]
    piece = cheight // groups
    chips = groups // 2
    reach = groups // 2
    chunk = margin // steps
    share = piece // parts

    flat = g * ranks + r
    has_left = flat > 0
    has_right = flat < groups * ranks - 1
    left = ((flat - 1) // ranks, (flat + ranks - 1) % ranks)
    right = ((flat + 1) // ranks, (flat + 1) % ranks)
    core = g % 2
    chip = g // 2
    partner = (chip * 2 + 1 - core, r)

    def piece_of(group, rank):
        odd = rank % 2
        return odd * (groups - 1 - group) + (1 - odd) * group

    q = piece_of(g, r)
    linear = r * groups + q

    def holder(index):
        rank = index // groups
        return (piece_of(index % groups, rank), rank)

    def chip_peer(o):
        return (((chip + o) % chips) * 2 + core, r)

    shifts = [d for s in range(1, reach + 1) for d in (s, -s)]

    def exists(index):
        return jnp.logical_and(index >= 0, index < groups * ranks)

    def load(src, dst, at):
        return pltpu.make_async_copy(src, dst, load_sem.at[at])

    mine = pl.ds(q * piece, piece)
    first_loads = [load(rhs_hbm, rhs, 0), load(smoother_hbm, smoother, 1)]
    later_loads = [
        load(blocks_hbm, blocks, 2),
        load(diag_hbm, diag, 3),
        load(csmoother_hbm.at[mine], csmoother, 4),
        load(cdiag_hbm.at[mine], cdiag, 5),
        load(cblocks_hbm.at[mine], cblocks, 6),
    ]
    for c in first_loads:
        c.start()

    barrier = pltpu.get_barrier_semaphore()

    def greet(device):
        pl.semaphore_signal(barrier, inc=1, device_id=device, device_id_type=MESH)

    pl.when(has_left)(lambda: greet(left))
    pl.when(has_right)(lambda: greet(right))
    greet(partner)
    for o in range(1, chips):
        greet(chip_peer(o))
    met = 1 + chips - 1 + has_left.astype(jnp.int32) + has_right.astype(jnp.int32)
    for d in shifts:
        there = exists(linear + d)
        pl.when(there)(functools.partial(lambda d: greet(holder(linear + d)), d))
        met = met + there.astype(jnp.int32)

    def remote(src, dst, send, recv, device):
        return pltpu.make_async_remote_copy(
            src_ref=src, dst_ref=dst, send_sem=send, recv_sem=recv, device_id=device, device_id_type=MESH
        )

    def to_right(ext, phase, j):
        src = ext.at[pl.ds(margin + height - (j + 1) * chunk, chunk)]
        at = pl.ds(margin - (j + 1) * chunk, chunk)
        dst = (landing1, landing2)[phase].at[0, at]
        return remote(src, dst, halo_send.at[phase, 0, j], halo_recv.at[phase, 0, j], right)

    def to_left(ext, phase, j):
        src = ext.at[pl.ds(margin + j * chunk, chunk)]
        at = pl.ds(j * chunk, chunk)
        dst = (landing1, landing2)[phase].at[1, at]
        return remote(src, dst, halo_send.at[phase, 1, j], halo_recv.at[phase, 1, j], left)

    def send_halo(ext, phase, j):
        pl.when(has_right)(lambda: to_right(ext, phase, j).start())
        pl.when(has_left)(lambda: to_left(ext, phase, j).start())

    def wait_halo(ext, phase, j):
        pl.when(has_left)(lambda: to_right(ext, phase, j).wait_recv())
        pl.when(has_right)(lambda: to_left(ext, phase, j).wait_recv())

    def wait_sent(ext, phase, j):
        pl.when(has_right)(lambda: to_right(ext, phase, j).wait_send())
        pl.when(has_left)(lambda: to_left(ext, phase, j).wait_send())

    def rows(start, count, body, unroll):
        def step(n, carry):
            body(start + n)
            return carry

        lax.fori_loop(0, count, step, 0, unroll=unroll)

    for c in first_loads:
        c.wait()
    for c in later_loads:
        c.start()

    def first(i):
        value = damping * dot(smoother[i], rhs[i].astype(low))
        iterate[i] = value
        ext1[margin + i] = value.astype(low)

    queue = [(ext1, 0, j) for j in range(steps)] + [(ext2, 1, steps - 1)] + [(ext2, 1, j) for j in range(steps - 1)]

    def push(n):
        if n >= depth:
            wait_sent(*queue[n - depth])
        send_halo(*queue[n])

    for j in range(steps):
        rows(height - (j + 1) * chunk, chunk, first, 4)
        rows(j * chunk, chunk, first, 4)
        if j == 1:
            pl.semaphore_wait(barrier, met)
            push(0)
            push(1)
        elif 1 < j < depth:
            push(j)
    starts = [at for j in range(steps) for at in (margin - (j + 1) * chunk, margin + j * chunk)]

    def earlier(wanted, runs):
        found = jnp.int32(0)
        for n in range(runs):
            for m in range(chunk):
                found = jnp.where(aggregate[starts[n] + m] == wanted, 1 + n * chunk + m, found)
        return found

    def link_run(n):
        def link(m):
            wanted = aggregate[starts[n] + m]
            found = earlier(wanted, n)
            for k in range(chunk - 1):
                same = jnp.logical_and(aggregate[starts[n] + k] == wanted, k < m)
                found = jnp.where(same, 1 + n * chunk + k, found)
            chain[starts[n] + m] = found

        rows(0, chunk, link, 1)

    def link_coarse(c):
        chain[height + c] = earlier(r * cheight + c, len(starts))

    def place(ext, landing, j):
        def place_low(i):
            ext[i] = landing[0, i]

        def place_high(i):
            ext[margin + height + i] = landing[1, i]

        pl.when(has_left)(lambda: rows(margin - (j + 1) * chunk, chunk, place_low, 4))
        pl.when(has_right)(lambda: rows(j * chunk, chunk, place_high, 4))

    rows(0, cheight // 2, link_coarse, 1)
    later_loads[0].wait()
    later_loads[1].wait()

    base = flat * height - margin

    def residual_low(i):
        residual = rhs[i] - row_product(i, fine_cols, i, base, blocks, diag, ext1, margin + i)
        ext2[margin + i] = residual.astype(low)

    def second(i):
        value = iterate[i] + damping * dot(smoother[i], ext2[margin + i])
        iterate[i] = value
        ext2[margin + i] = value.astype(low)

    for j in range(steps):
        if j + depth <= steps:
            push(j + depth)
        wait_halo(ext1, 0, j)
        place(ext1, landing1, j)
        rows(margin - (j + 1) * chunk, chunk, residual_low, 4)
        rows(margin + j * chunk, chunk, residual_low, 4)
        rows(margin - (j + 1) * chunk, chunk, second, 4)
        rows(margin + j * chunk, chunk, second, 4)
        if j < steps - 1:
            link_run(2 * j)
            link_run(2 * j + 1)
    for n in range(steps + 1, steps + depth):
        push(n)
    keep_iterate = pltpu.make_async_copy(iterate, iterate_hbm, load_sem.at[7])
    keep_iterate.start()
    link_run(2 * steps - 2)
    link_run(2 * steps - 1)

    sums[0] = jnp.zeros(sums.shape[1:], f32)

    def third(shift):
        def body(i):
            residual = rhs[i] - row_product(i, fine_cols, i, base, blocks, diag, ext2, margin + i)
            sums[i + shift] = residual + sums[chain[i]]

        return body

    wait_halo(ext2, 1, steps - 1)
    place(ext2, landing2, steps - 1)
    for j in range(steps):
        if steps + depth + j < 2 * steps:
            push(steps + depth + j)
        if j < steps - 1:
            wait_halo(ext2, 1, j)
            place(ext2, landing2, j)
        for n, start in enumerate((margin - (j + 1) * chunk, margin + j * chunk)):
            rows(start, chunk, third(1 + (2 * j + n) * chunk - start), 2)
        if j < 4:
            rows(cheight // 2 + j * (cheight // 8), cheight // 8, link_coarse, 1)

    def gather(c):
        partial[c] = sums[chain[height + c]]

    rows(0, cheight, gather, 4)

    def slice_of(group, p):
        return pl.ds(piece_of(group, r) * piece + p * share, share)

    def to_partner(o, p):
        src = partial.at[slice_of(((chip + o) % chips) * 2 + 1 - core, p)]
        dst = from_partner.at[o, pl.ds(p * share, share)]
        return remote(src, dst, rs_send.at[o, p], rs_recv.at[o, p], partner)

    order = [*range(1, chips), 0]
    for o in order:
        for p in range(parts):
            to_partner(o, p).start()

    def across(o, p):
        at = pl.ds(p * share, share)
        return remote(chip_send.at[o, at], chip_recv.at[o, at], rc_send.at[o, p], rc_recv.at[o, p], chip_peer(o))

    for o in order:
        start = piece_of(((chip + o) % chips) * 2 + core, r) * piece

        def pack(n):
            chip_send[o, n] = (partial[start + n] + from_partner[o, n]).astype(low)

        def keep(n):
            crhs[n] = partial[start + n] + from_partner[o, n]

        for p in range(parts):
            to_partner(o, p).wait_recv()
            rows(p * share, share, pack if o else keep, 2)
            if o:
                across(o, p).start()
    for c in later_loads[2:]:
        c.wait()

    def coarse_first(n):
        total = crhs[n]
        for o in range(1, chips):
            total = total + chip_recv[o, n].astype(f32)
        crhs[n] = total
        value = damping * dot(csmoother[n], total.astype(low))
        cfirst[n] = value
        cext[reach * piece + n] = value.astype(low)

    def to_shift(d, p):
        at = shifts.index(d)
        return remote(
            cext.at[pl.ds(reach * piece + p * share, share)], cext.at[pl.ds((reach - d) * piece + p * share, share)],
            piece_send.at[at, p], piece_recv.at[at, p], holder(linear + d),
        )

    def each_part(method, d):
        for p in range(parts):
            getattr(to_shift(d, p), method)()

    for p in range(parts):
        for o in range(1, chips):
            across(o, p).wait_recv()
        rows(p * share, share, coarse_first, 2)
        for d in reversed(shifts):
            pl.when(exists(linear + d))(functools.partial(lambda d: to_shift(d, p).start(), d))
    for d in reversed(shifts):
        pl.when(exists(linear - d))(functools.partial(each_part, "wait_recv", d))

    cbase = (linear - reach) * piece

    def coarse_second(n):
        image = row_product(n, coarse_cols, q * piece + n, cbase, cblocks, cdiag, cext, reach * piece + n)
        value = cfirst[n] + damping * dot(csmoother[n], (crhs[n] - image).astype(low))
        correction[q * piece + n] = value.astype(low)

    def piece_to(o, p):
        at = slice_of(g, p)
        return remote(correction.at[at], correction.at[at], ag_send.at[o, p], ag_recv.at[o, p], chip_peer(o))

    def forward(o, p):
        at = slice_of(((chip + o) % chips) * 2 + core, p)
        return remote(correction.at[at], correction.at[at], fwd_send.at[o, p], fwd_recv.at[o, p], partner)

    def put(o, own, p):
        at = slice_of(((chip + o) % chips) * 2 + (core if own else 1 - core), p)
        return pltpu.make_async_copy(correction.at[at], correction_hbm.at[at], out_sem.at[o, own, p])

    for p in range(parts):
        rows(p * share, share, coarse_second, 2)
        for o in range(1, chips):
            piece_to(o, p).start()
        forward(0, p).start()
        put(0, 1, p).start()
    for o in range(1, chips):
        for p in range(parts):
            piece_to(o, p).wait_recv()
            forward(chips - o, p).start()
            put(chips - o, 1, p).start()
    for o in [0, *reversed(range(1, chips))]:
        for p in range(parts):
            forward(o, p).wait_recv()
            put(o, 0, p).start()

    for n in range(2 * steps - depth, 2 * steps):
        wait_sent(*queue[n])
    for p in range(parts):
        for o in range(chips):
            to_partner(o, p).wait_send()
            forward(o, p).wait_send()
            put(o, 0, p).wait()
            put(o, 1, p).wait()
        for o in range(1, chips):
            across(o, p).wait_send()
            piece_to(o, p).wait_send()
    for d in shifts:
        pl.when(exists(linear + d))(functools.partial(each_part, "wait_send", d))
    keep_iterate.wait()


def add_kernel(
    cheight, aggregate, iterate_hbm, correction_hbm, out_hbm, iterate, correction, in_sem, correction_sem, out_sem
):
    share = iterate.shape[0] // 4
    cshare = cheight // 4
    start = lax.axis_index("rows") * cheight

    def fetch(j):
        at = pl.ds(j * cshare, cshare)
        return pltpu.make_async_copy(correction_hbm.at[at], correction.at[at], correction_sem.at[j])

    def get(j):
        at = pl.ds(j * share, share)
        return pltpu.make_async_copy(iterate_hbm.at[at], iterate.at[at], in_sem.at[j])

    def put(j):
        at = pl.ds(j * share, share)
        return pltpu.make_async_copy(iterate.at[at], out_hbm.at[at], out_sem.at[j])

    for j in range(4):
        fetch(j).start()
    for j in range(4):
        get(j).start()
    for j in range(4):
        fetch(j).wait()
    for j in range(4):
        get(j).wait()

        def step(n, carry):
            i = j * share + n
            iterate[i] = iterate[i] + correction[aggregate[i] - start].astype(f32)
            return carry

        lax.fori_loop(0, share, step, 0, unroll=4)
        put(j).start()
    for j in range(4):
        put(j).wait()


def on_device(
    groups, ranks,
    rhs, fine_diag, fine_smoother, fine_blocks, fine_cols, aggregate,
    coarse_diag, coarse_smoother, coarse_blocks, coarse_cols,
):
    height, b, n = rhs.shape
    cheight = coarse_diag.shape[0]
    neighbours = fine_blocks.shape[1]
    piece = cheight // groups
    chips = groups // 2
    reach = groups // 2
    vmem = pltpu.VMEM
    dma = pltpu.SemaphoreType.DMA
    smem = pl.BlockSpec(memory_space=pltpu.SMEM)
    hbm = pl.BlockSpec(memory_space=pl.ANY)
    iterate, correction = pl.pallas_call(
        functools.partial(kernel, groups, ranks),
        out_shape=(jax.ShapeDtypeStruct(rhs.shape, f32), jax.ShapeDtypeStruct((cheight, b, n), low)),
        in_specs=[smem] * 3 + [hbm] * 7,
        out_specs=(hbm, hbm),
        scratch_shapes=[
            vmem((height, b, n), f32),
            vmem((height, b, b), low),
            vmem((height, b, b), low),
            vmem((height, neighbours, b, b), low),
            vmem((piece, b, b), low),
            vmem((piece, b, b), low),
            vmem((piece, neighbours, b, b), low),
            vmem((2 * height, b, n), low),
            vmem((2 * height, b, n), low),
            vmem((2, height // 2, b, n), low),
            vmem((2, height // 2, b, n), low),
            vmem((height, b, n), f32),
            vmem((height + 1, b, n), f32),
            vmem((cheight, b, n), f32),
            vmem((chips, piece, b, n), f32),
            vmem((chips, piece, b, n), low),
            vmem((chips, piece, b, n), low),
            vmem((piece, b, n), f32),
            vmem((piece, b, n), f32),
            vmem(((2 * reach + 1) * piece, b, n), low),
            vmem((cheight, b, n), low),
            pltpu.SMEM((height + cheight,), jnp.int32),
            dma((8,)),
            dma((chips, 2, parts)),
            dma((2, 2, steps)),
            dma((2, 2, steps)),
            dma((chips, parts)),
            dma((chips, parts)),
            dma((chips, parts)),
            dma((chips, parts)),
            dma((2 * reach, parts)),
            dma((2 * reach, parts)),
            dma((chips, parts)),
            dma((chips, parts)),
            dma((chips, parts)),
            dma((chips, parts)),
        ],
        compiler_params=pltpu.CompilerParams(
            collective_id=0, has_side_effects=True, vmem_limit_bytes=60 * 1024 * 1024
        ),
        name="cycle",
    )(
        fine_cols.T, coarse_cols.T, aggregate,
        rhs, fine_diag, fine_smoother, fine_blocks, coarse_diag, coarse_smoother, coarse_blocks,
    )
    return pl.pallas_call(
        functools.partial(add_kernel, cheight),
        out_shape=jax.ShapeDtypeStruct(rhs.shape, f32),
        in_specs=[smem, hbm, hbm],
        out_specs=hbm,
        scratch_shapes=[vmem((height, b, n), f32), vmem((cheight, b, n), low), dma((4,)), dma((4,)), dma((4,))],
        name="add",
    )(aggregate, iterate, correction)


def solution(mesh):
    fine = P(("grp", "rows"))
    return jax.shard_map(
        functools.partial(on_device, mesh.shape["grp"], mesh.shape["rows"]),
        mesh=mesh,
        in_specs=(fine,) * 6 + (P("rows"),) * 4,
        out_specs=fine,
        check_vma=False,
    )
```

```python
import functools

import jax
import jax.numpy as jnp
from jax import lax
from jax.experimental import pallas as pl
from jax.experimental.pallas import tpu as pltpu
from jax.sharding import PartitionSpec as P

MESH = pl.DeviceIdType.MESH
damping = 0.8
lanes = 128
sublanes = 8
depth = 4
csub = 4
low = jnp.bfloat16
f32 = jnp.float32


def dot(a, b):
    return jnp.dot(a, b, preferred_element_type=f32)


def row_product(i, columns, at, base, offs, diag, extended, own):
    count = offs.shape[1]
    last = extended.shape[0] - 1
    vectors = [extended[jnp.clip(columns[k, at] - base, 0, last)] for k in range(count)] + [extended[own]]
    blocks = [offs[i, k] for k in range(count)] + [diag[i]]
    total = None
    for p in range(0, count + 1, 4):
        term = dot(
            jnp.concatenate(blocks[p : p + 4], axis=1),
            jnp.concatenate(vectors[p : p + 4], axis=0),
        )
        total = term if total is None else total + term
    return total


def absorb_order(groups, steps):
    lag = [0, 1] + [4 + k % 2 for k in range(2, groups)]
    return [(k, t - lag[k]) for t in range(steps + max(lag)) for k in range(groups) if 0 <= t - lag[k] < steps]


def kernel(
    groups, ranks,
    fine_cols, coarse_cols, aggregate,
    rhs_hbm, diag_hbm, smoother_hbm, blocks_hbm, cdiag_hbm, csmoother_hbm, cblocks_hbm,
    iterate,
    rhs, diag, smoother, blocks, cdiag, csmoother, cblocks,
    ext1, ext2, landing1, landing2,
    own_full, own_low, near_full, far_low, via_low, sums, names, tables, chain,
    cfirst, cres, cext, clanding, correction,
    load_sem, halo_send, halo_recv, name_sem, near_send, near_recv,
    far_send, far_recv, via_send, via_recv, cx_send, cx_recv, cf_send, cf_recv, cp_sem,
):
    g = lax.axis_index("grp")
    r = lax.axis_index("rows")
    height = rhs.shape[0]
    margin = height // 2
    steps = height // sublanes
    chunk = sublanes // 2
    piece = chunk // 2
    cheight = correction.shape[0]
    cmargin = cheight // 2
    chips = groups // 2
    parts = cmargin // (csub * chips)
    span = csub * chips

    flat = g * ranks + r
    has_left = flat > 0
    has_right = flat < groups * ranks - 1
    left = ((flat - 1) // ranks, (flat + ranks - 1) % ranks)
    right = ((flat + 1) // ranks, (flat + 1) % ranks)
    core = g % 2
    chip = g // 2
    partner = (chip * 2 + 1 - core, r)
    side = 1 - core
    forth = (g, r + 1 - 2 * core)
    can_send = jnp.where(core == 0, r < ranks - 1, r > 0)
    can_recv = jnp.where(core == 0, r > 0, r < ranks - 1)

    def peer(o, same):
        return (((chip + o) % chips) * 2 + (core if same else 1 - core), r)

    def load(src, dst, at):
        return pltpu.make_async_copy(src, dst, load_sem.at[at])

    mine = pl.ds(core * cmargin, cmargin)
    first_loads = [load(rhs_hbm, rhs, 0), load(smoother_hbm, smoother, 1)]
    later_loads = [
        load(blocks_hbm, blocks, 2),
        load(diag_hbm, diag, 3),
        load(csmoother_hbm, csmoother, 4),
        load(cdiag_hbm.at[mine], cdiag, 5),
        load(cblocks_hbm.at[mine], cblocks, 6),
    ]
    for c in first_loads:
        c.start()

    barrier = pltpu.get_barrier_semaphore()

    def greet(device):
        pl.semaphore_signal(barrier, inc=1, device_id=device, device_id_type=MESH)

    pl.when(has_left)(lambda: greet(left))
    pl.when(has_right)(lambda: greet(right))
    greet(partner)
    for o in range(1, chips):
        greet(peer(o, True))
        greet(peer(o, False))
    met = groups - 1 + has_left.astype(jnp.int32) + has_right.astype(jnp.int32)

    def remote(src, dst, send, recv, device):
        return pltpu.make_async_remote_copy(
            src_ref=src, dst_ref=dst, send_sem=send, recv_sem=recv, device_id=device, device_id_type=MESH
        )

    pieces = margin // piece
    queue = [(0, j * piece, piece) for j in range(pieces)] + [(1, margin - piece, piece)]
    queue += [(1, j * piece, piece) for j in range(pieces - 1)]
    second_queue = pieces + 1
    pushed = []
    exts, landings = (ext1, ext2), (landing1, landing2)

    def to_right(n, item=None):
        phase, start, count = item or queue[n]
        src = exts[phase].at[pl.ds(margin + height - start - count, count)]
        dst = landings[phase].at[0, pl.ds(margin - start - count, count)]
        return remote(src, dst, halo_send.at[0, n % depth], halo_recv.at[phase, 0, start // chunk], right)

    def to_left(n, item=None):
        phase, start, count = item or queue[n]
        src = exts[phase].at[pl.ds(margin + start, count)]
        dst = landings[phase].at[1, pl.ds(start, count)]
        return remote(src, dst, halo_send.at[1, n % depth], halo_recv.at[phase, 1, start // chunk], left)

    def wait_sent(n):
        pl.when(has_right)(lambda: to_right(n).wait_send())
        pl.when(has_left)(lambda: to_left(n).wait_send())

    def launch(n):
        if n >= depth:
            wait_sent(n - depth)
        pl.when(has_right)(lambda: to_right(n).start())
        pl.when(has_left)(lambda: to_left(n).start())

    def push(upto):
        while len(pushed) < min(upto, len(queue)):
            launch(len(pushed))
            pushed.append(None)

    def rows(start, count, body, unroll):
        def step(n, carry):
            body(start + n)
            return carry

        lax.fori_loop(0, count, step, 0, unroll=unroll)

    def wait_halo(phase, j):
        start, count = j * chunk, chunk
        pl.when(has_left)(lambda: to_right(0, (phase, start, count)).wait_recv())
        pl.when(has_right)(lambda: to_left(0, (phase, start, count)).wait_recv())
        ext, landing = exts[phase], landings[phase]

        def place_low(i):
            ext[i] = landing[0, i]

        def place_high(i):
            ext[margin + height + i] = landing[1, i]

        pl.when(has_left)(lambda: rows(margin - start - count, count, place_low, count))
        pl.when(has_right)(lambda: rows(start, count, place_high, count))

    starts = [at for j in range(steps) for at in (margin - (j + 1) * chunk, margin + j * chunk)]

    lane = lax.broadcasted_iota(jnp.int32, (sublanes, lanes), 1)
    sublane = lax.broadcasted_iota(jnp.int32, (sublanes, lanes), 0)
    named = jnp.zeros((sublanes, lanes), jnp.int32)
    for n, start in enumerate(starts):
        for m in range(chunk):
            named = jnp.where(lane == n * chunk + m, aggregate[start + m], named)
    names[0] = named

    def name_copies():
        yield remote(names.at[0], names.at[1], name_sem.at[0], name_sem.at[1], partner)
        for o in range(1, chips):
            for other in (0, 1):
                yield remote(names.at[0], names.at[2 * o + other], name_sem.at[0], name_sem.at[1], peer(o, not other))

    others = names.at[pl.ds(1, groups - 1)]
    all_names = remote(others, others, name_sem.at[0], name_sem.at[1], partner)

    for c in first_loads:
        c.wait()
    for c in later_loads:
        c.start()

    def first(i):
        value = damping * dot(smoother[i], rhs[i].astype(low))
        iterate[i] = value
        ext1[margin + i] = value.astype(low)

    for j in range(steps):
        rows(height - (j + 1) * chunk, chunk, first, 4)
        rows(j * chunk, chunk, first, 4)
        if j == 1:
            pl.semaphore_wait(barrier, met)
            push(depth)
            for c in name_copies():
                c.start()

    order = absorb_order(groups, steps)
    place_of = {key: 1 + sublanes * n for n, key in enumerate(order)}
    all_names.wait_recv()
    columns = jnp.zeros((sublanes, lanes), jnp.int32)
    places = []
    for k in range(groups):
        columns = jnp.where(sublane == k, names[k], columns)
        spot = lane % sublanes
        for j in range(steps):
            spot = jnp.where(lane // sublanes == j, spot + place_of[k, j], spot)
        places.append(spot)
    columns = columns.T
    found = [jnp.zeros((sublanes, lanes), jnp.int32) for _ in range(groups + 1)]
    for k in range(groups):
        for j in range(steps):
            column = jnp.broadcast_to(columns[sublanes * j : sublanes * (j + 1), k : k + 1], (sublanes, lanes))
            spot = place_of[k, j] + sublane
            for i in range(groups):
                hit = jnp.logical_and(column == names[i], spot < places[i])
                found[i] = jnp.maximum(found[i], jnp.where(hit, spot, 0))
            hit = column == r * cheight + lane
            found[groups] = jnp.maximum(found[groups], jnp.where(hit, spot, 0))
    for i in range(groups + 1):
        best = found[i]
        for shift in (1, 2, 4):
            best = jnp.maximum(best, pltpu.roll(best, shift, 0))
        tables[pl.ds(sublanes * i, sublanes)] = best
    to_scalar = load(tables, chain, 7)
    to_scalar.start()
    sums[0] = jnp.zeros(sums.shape[1:], f32)
    to_scalar.wait()
    later_loads[0].wait()
    later_loads[1].wait()

    base = flat * height - margin

    def residual_low(i):
        residual = rhs[i] - row_product(i, fine_cols, i, base, blocks, diag, ext1, margin + i)
        ext2[margin + i] = residual.astype(low)

    def second(i):
        value = iterate[i] + damping * dot(smoother[i], ext2[margin + i])
        iterate[i] = value
        ext2[margin + i] = value.astype(low)

    for j in range(steps):
        push(min(2 * j + 2 + depth, second_queue))
        wait_halo(0, j)
        for body in (residual_low, second):
            rows(margin - (j + 1) * chunk, chunk, body, 4)
            rows(margin + j * chunk, chunk, body, 4)
    push(second_queue + depth)

    def third(shift, spot):
        def body(i):
            at = i + shift
            residual = rhs[i] - row_product(i, fine_cols, i, base, blocks, diag, ext2, margin + i)
            own_full[at] = residual
            own_low[at] = residual.astype(low)
            sums[at + spot] = residual + sums[chain[0, at]]

        return body

    def near(j, count=sublanes):
        at = pl.ds(j * sublanes, count)
        return remote(own_full.at[at], near_full.at[at], near_send.at[0], near_recv.at[j], partner)

    def far(o, j, count=sublanes):
        at = pl.ds(j * sublanes, count)
        return remote(own_low.at[at], far_low.at[o - 1, at], far_send.at[o - 1], far_recv.at[o - 1, j], peer(o, True))

    def via(o, j, count=sublanes):
        at = pl.ds(j * sublanes, count)
        return remote(
            far_low.at[o - 1, at], via_low.at[o - 1, at], via_send.at[o - 1], via_recv.at[o - 1, j], partner
        )

    def absorb(k, j):
        source = near_full if k == 1 else (via_low if k % 2 else far_low).at[k // 2 - 1]
        spot = place_of[k, j] - j * sublanes

        def body(at):
            sums[at + spot] = source[at].astype(f32) + sums[chain[sublanes * k, at]]

        rows(j * sublanes, sublanes, body, 4)

    for k, j in order:
        o = k // 2
        if k == 0:
            push(second_queue + 2 * j + 2 + depth)
            wait_halo(1, j)
            for n in (0, 1):
                start, at = starts[2 * j + n], (2 * j + n) * chunk
                rows(start, chunk, third(at - start, place_of[k, j] - j * sublanes), 2)
            for o in range(1, chips):
                far(o, j).start()
            near(j).start()
        elif k == 1:
            near(j).wait_recv()
            absorb(k, j)
        elif k % 2 == 0:
            far(o, j).wait_recv()
            via(o, j).start()
            absorb(k, j)
        else:
            via(o, j).wait_recv()
            absorb(k, j)
    for c in later_loads[2:]:
        c.wait()

    def coarse_first(c):
        value = damping * dot(csmoother[c], sums[chain[sublanes * groups, c]].astype(low))
        cfirst[c] = value
        cext[cmargin + c] = value.astype(low)

    def spot_of(u):
        return side * (cmargin - (u + 1) * csub) + core * u * csub

    def across(p):
        at = spot_of(p * chips + chip)
        src = cext.at[pl.ds(cmargin + side * cmargin + at, csub)]
        return remote(src, clanding.at[pl.ds(at, csub)], cx_send.at[0], cx_recv.at[p], forth)

    def forward(o, p):
        at = pl.ds(spot_of(p * chips + chip), csub)
        return remote(clanding.at[at], clanding.at[at], cf_send.at[o - 1], cf_recv.at[o - 1, p], peer(o, True))

    for p in range(parts):
        rows(side * cmargin + spot_of(p * chips + chip), csub, coarse_first, csub)
        pl.when(can_send)(lambda: across(p).start())
    for p in range(parts):
        for o in range(1, chips):
            rows(side * cmargin + spot_of(p * chips + (chip + o) % chips), csub, coarse_first, csub)
    rows(core * cmargin, cmargin, coarse_first, 4)

    cbase = r * cheight - cmargin
    own = core * cmargin

    def coarse_residual(n):
        image = row_product(n, coarse_cols, own + n, cbase, cblocks, cdiag, cext, cmargin + own + n)
        cres[n] = (sums[chain[sublanes * groups, own + n]] - image).astype(low)

    def coarse_second(n):
        correction[own + n] = cfirst[own + n] + damping * dot(csmoother[own + n], cres[n])

    def back(p):
        at = pl.ds(own + side * (cmargin - (p + 1) * span) + core * p * span, span)
        return remote(correction.at[at], correction.at[at], cp_sem.at[0], cp_sem.at[1], partner)

    halves = correction.at[mine]
    all_back = remote(halves, halves, cp_sem.at[0], cp_sem.at[1], partner)
    sent = clanding.at[pl.ds(0, parts * csub)]
    all_across = remote(sent, sent, cx_send.at[0], cx_recv.at[0], forth)
    all_forward = [remote(sent, sent, cf_send.at[o - 1], cf_recv.at[o - 1, 0], peer(o, True)) for o in range(1, chips)]

    def receive(p):
        def go():
            across(p).wait_recv()
            for o in range(1, chips):
                forward(o, p).start()

        pl.when(can_recv)(go)

    receive(0)
    for p in range(parts):
        if p + 1 < parts:
            receive(p + 1)
        begin = side * (cmargin - (p + 1) * span) + core * p * span

        def arrived():
            for o in range(1, chips):
                forward(o, p).wait_recv()

            def place(n):
                cext[core * (cmargin + cheight) + n] = clanding[n]

            rows(begin, span, place, 4)

        pl.when(can_recv)(arrived)
        rows(begin, span, coarse_residual, 4)
        rows(begin, span, coarse_second, 4)
        back(p).start()
    all_back.wait_recv()

    cstart = r * cheight

    def final(i):
        iterate[i] = iterate[i] + correction[jnp.clip(aggregate[i] - cstart, 0, cheight - 1)]

    rows(0, height, final, 4)

    for n in range(len(queue) - depth, len(queue)):
        wait_sent(n)
    all_names.wait_send()
    near(0, height).wait_send()
    for o in range(1, chips):
        far(o, 0, height).wait_send()
        via(o, 0, height).wait_send()

    for c in all_forward:
        pl.when(can_recv)(lambda: c.wait_send())
    pl.when(can_send)(lambda: all_across.wait_send())
    all_back.wait_send()


def on_device(
    groups, ranks,
    rhs, fine_diag, fine_smoother, fine_blocks, fine_cols, aggregate,
    coarse_diag, coarse_smoother, coarse_blocks, coarse_cols,
):
    height, b, n = rhs.shape
    cheight = coarse_diag.shape[0]
    cmargin = cheight // 2
    neighbours = fine_blocks.shape[1]
    chips = groups // 2
    steps = height // sublanes
    parts = cmargin // (csub * chips)
    vmem = pltpu.VMEM
    dma = pltpu.SemaphoreType.DMA
    smem = pl.BlockSpec(memory_space=pltpu.SMEM)
    hbm = pl.BlockSpec(memory_space=pl.ANY)
    return pl.pallas_call(
        functools.partial(kernel, groups, ranks),
        out_shape=pltpu.VMEM(rhs.shape, f32),
        in_specs=[smem] * 3 + [hbm] * 7,
        out_specs=pl.BlockSpec(memory_space=pltpu.VMEM),
        scratch_shapes=[
            vmem((height, b, n), f32),
            vmem((height, b, b), low),
            vmem((height, b, b), low),
            vmem((height, neighbours, b, b), low),
            vmem((cmargin, b, b), low),
            vmem((cheight, b, b), low),
            vmem((cmargin, neighbours, b, b), low),
            vmem((2 * height, b, n), low),
            vmem((2 * height, b, n), low),
            vmem((2, height // 2, b, n), low),
            vmem((2, height // 2, b, n), low),
            vmem((height, b, n), f32),
            vmem((height, b, n), low),
            vmem((height, b, n), f32),
            vmem((chips - 1, height, b, n), low),
            vmem((chips - 1, height, b, n), low),
            vmem((groups * height + 1, b, n), f32),
            vmem((groups, sublanes, lanes), jnp.int32),
            vmem(((groups + 1) * sublanes, lanes), jnp.int32),
            pltpu.SMEM(((groups + 1) * sublanes, lanes), jnp.int32),
            vmem((cheight, b, n), f32),
            vmem((cmargin, b, n), low),
            vmem((2 * cheight, b, n), low),
            vmem((cmargin, b, n), low),
            vmem((cheight, b, n), f32),
            dma((8,)),
            dma((2, depth)),
            dma((2, 2, steps)),
            dma((2,)),
            dma((1,)),
            dma((steps,)),
            dma((chips - 1,)),
            dma((chips - 1, steps)),
            dma((chips - 1,)),
            dma((chips - 1, steps)),
            dma((1,)),
            dma((parts,)),
            dma((chips - 1,)),
            dma((chips - 1, parts)),
            dma((2,)),
        ],
        compiler_params=pltpu.CompilerParams(
            collective_id=0, has_side_effects=True, vmem_limit_bytes=58 * 1024 * 1024
        ),
        name="cycle",
    )(
        fine_cols.T, coarse_cols.T, aggregate,
        rhs, fine_diag, fine_smoother, fine_blocks, coarse_diag, coarse_smoother, coarse_blocks,
    )


def solution(mesh):
    fine = P(("grp", "rows"))
    return jax.shard_map(
        functools.partial(on_device, mesh.shape["grp"], mesh.shape["rows"]),
        mesh=mesh,
        in_specs=(fine,) * 6 + (P("rows"),) * 4,
        out_specs=fine,
        check_vma=False,
    )
```

```python
import functools

import jax
import jax.numpy as jnp
from jax import lax
from jax.experimental import pallas as pl
from jax.experimental.pallas import tpu as pltpu
from jax.sharding import PartitionSpec as P

MESH = pl.DeviceIdType.MESH
damping = 0.8
lanes = 128
sublanes = 8
depth = 4
csub = 2
low = jnp.bfloat16
f32 = jnp.float32


def dot(a, b):
    return jnp.dot(a, b, preferred_element_type=f32)


def row_product(i, columns, at, base, offs, diag, extended, own):
    count = offs.shape[1]
    last = extended.shape[0] - 1
    vectors = [extended[jnp.clip(columns[k, at] - base, 0, last)] for k in range(count)] + [extended[own]]
    blocks = [offs[i, k] for k in range(count)] + [diag[i]]
    total = None
    for p in range(0, count + 1, 4):
        term = dot(
            jnp.concatenate(blocks[p : p + 4], axis=1),
            jnp.concatenate(vectors[p : p + 4], axis=0),
        )
        total = term if total is None else total + term
    return total


def absorb_order(groups, steps):
    lag = [0, 1] + [4 + k % 2 for k in range(2, groups)]
    return [(k, t - lag[k]) for t in range(steps + max(lag)) for k in range(groups) if 0 <= t - lag[k] < steps]


def kernel(
    groups, ranks,
    fine_cols, coarse_cols, aggregate,
    rhs_hbm, diag_hbm, smoother_hbm, blocks_hbm, cdiag_hbm, csmoother_hbm, cblocks_hbm,
    iterate,
    rhs, diag, smoother, blocks, cdiag, csmoother, cblocks,
    ext1, ext2, landing1, landing2,
    own_full, own_low, near_full, far_low, via_low, sums, names, tables, chain,
    cfirst, cres, cext, clanding, correction,
    load_sem, halo_send, halo_recv, name_sem, near_send, near_recv,
    far_send, far_recv, via_send, via_recv, cx_send, cx_recv, cf_send, cf_recv, cp_sem,
):
    g = lax.axis_index("grp")
    r = lax.axis_index("rows")
    height = rhs.shape[0]
    margin = height // 2
    steps = height // sublanes
    chunk = sublanes // 2
    piece = chunk // 2
    cheight = correction.shape[0]
    cmargin = cheight // 2
    chips = groups // 2
    parts = cmargin // (csub * chips)
    span = csub * chips

    flat = g * ranks + r
    has_left = flat > 0
    has_right = flat < groups * ranks - 1
    left = ((flat - 1) // ranks, (flat + ranks - 1) % ranks)
    right = ((flat + 1) // ranks, (flat + 1) % ranks)
    core = g % 2
    chip = g // 2
    partner = (chip * 2 + 1 - core, r)
    side = 1 - core
    forth = (g, r + 1 - 2 * core)
    can_send = jnp.where(core == 0, r < ranks - 1, r > 0)
    can_recv = jnp.where(core == 0, r > 0, r < ranks - 1)

    def peer(o, same):
        return (((chip + o) % chips) * 2 + (core if same else 1 - core), r)

    def load(src, dst, at):
        return pltpu.make_async_copy(src, dst, load_sem.at[at])

    mine = pl.ds(core * cmargin, cmargin)
    first_loads = [load(rhs_hbm, rhs, 0), load(smoother_hbm, smoother, 1)]
    later_loads = [
        load(blocks_hbm, blocks, 2),
        load(diag_hbm, diag, 3),
        load(csmoother_hbm, csmoother, 4),
        load(cdiag_hbm.at[mine], cdiag, 5),
        load(cblocks_hbm.at[mine], cblocks, 6),
    ]
    for c in first_loads:
        c.start()

    barrier = pltpu.get_barrier_semaphore()

    def greet(device):
        pl.semaphore_signal(barrier, inc=1, device_id=device, device_id_type=MESH)

    pl.when(has_left)(lambda: greet(left))
    pl.when(has_right)(lambda: greet(right))
    greet(partner)
    for o in range(1, chips):
        greet(peer(o, True))
        greet(peer(o, False))
    met = groups - 1 + has_left.astype(jnp.int32) + has_right.astype(jnp.int32)

    def remote(src, dst, send, recv, device):
        return pltpu.make_async_remote_copy(
            src_ref=src, dst_ref=dst, send_sem=send, recv_sem=recv, device_id=device, device_id_type=MESH
        )

    pieces = margin // piece
    queue = [(0, j * piece, piece) for j in range(pieces)] + [(1, margin - piece, piece)]
    queue += [(1, j * piece, piece) for j in range(pieces - 1)]
    second_queue = pieces + 1
    pushed = []
    exts, landings = (ext1, ext2), (landing1, landing2)

    def to_right(n, item=None):
        phase, start, count = item or queue[n]
        src = exts[phase].at[pl.ds(margin + height - start - count, count)]
        dst = landings[phase].at[0, pl.ds(margin - start - count, count)]
        return remote(src, dst, halo_send.at[0, n % depth], halo_recv.at[phase, 0, start // chunk], right)

    def to_left(n, item=None):
        phase, start, count = item or queue[n]
        src = exts[phase].at[pl.ds(margin + start, count)]
        dst = landings[phase].at[1, pl.ds(start, count)]
        return remote(src, dst, halo_send.at[1, n % depth], halo_recv.at[phase, 1, start // chunk], left)

    def wait_sent(n):
        pl.when(has_right)(lambda: to_right(n).wait_send())
        pl.when(has_left)(lambda: to_left(n).wait_send())

    def launch(n):
        if n >= depth:
            wait_sent(n - depth)
        pl.when(has_right)(lambda: to_right(n).start())
        pl.when(has_left)(lambda: to_left(n).start())

    def push(upto):
        while len(pushed) < min(upto, len(queue)):
            launch(len(pushed))
            pushed.append(None)

    def rows(start, count, body, unroll):
        def step(n, carry):
            body(start + n)
            return carry

        lax.fori_loop(0, count, step, 0, unroll=unroll)

    def wait_halo(phase, j):
        start, count = j * chunk, chunk
        pl.when(has_left)(lambda: to_right(0, (phase, start, count)).wait_recv())
        pl.when(has_right)(lambda: to_left(0, (phase, start, count)).wait_recv())
        ext, landing = exts[phase], landings[phase]

        def place_low(i):
            ext[i] = landing[0, i]

        def place_high(i):
            ext[margin + height + i] = landing[1, i]

        pl.when(has_left)(lambda: rows(margin - start - count, count, place_low, count))
        pl.when(has_right)(lambda: rows(start, count, place_high, count))

    starts = [at for j in range(steps) for at in (margin - (j + 1) * chunk, margin + j * chunk)]

    lane = lax.broadcasted_iota(jnp.int32, (sublanes, lanes), 1)
    sublane = lax.broadcasted_iota(jnp.int32, (sublanes, lanes), 0)
    named = jnp.zeros((sublanes, lanes), jnp.int32)
    for n, start in enumerate(starts):
        for m in range(chunk):
            named = jnp.where(lane == n * chunk + m, aggregate[start + m], named)
    names[0] = named

    def name_copies():
        yield remote(names.at[0], names.at[1], name_sem.at[0], name_sem.at[1], partner)
        for o in range(1, chips):
            for other in (0, 1):
                yield remote(names.at[0], names.at[2 * o + other], name_sem.at[0], name_sem.at[1], peer(o, not other))

    others = names.at[pl.ds(1, groups - 1)]
    all_names = remote(others, others, name_sem.at[0], name_sem.at[1], partner)

    for c in first_loads:
        c.wait()
    for c in later_loads:
        c.start()

    def first(i):
        value = damping * dot(smoother[i], rhs[i].astype(low))
        iterate[i] = value
        ext1[margin + i] = value.astype(low)

    for j in range(steps):
        rows(height - (j + 1) * chunk, chunk, first, 4)
        rows(j * chunk, chunk, first, 4)
        if j == 1:
            pl.semaphore_wait(barrier, met)
            push(depth)
            for c in name_copies():
                c.start()

    order = absorb_order(groups, steps)
    place_of = {key: 1 + sublanes * n for n, key in enumerate(order)}
    all_names.wait_recv()
    columns = jnp.zeros((sublanes, lanes), jnp.int32)
    places = []
    for k in range(groups):
        columns = jnp.where(sublane == k, names[k], columns)
        spot = lane % sublanes
        for j in range(steps):
            spot = jnp.where(lane // sublanes == j, spot + place_of[k, j], spot)
        places.append(spot)
    columns = columns.T
    found = [jnp.zeros((sublanes, lanes), jnp.int32) for _ in range(groups + 1)]
    for k in range(groups):
        for j in range(steps):
            column = jnp.broadcast_to(columns[sublanes * j : sublanes * (j + 1), k : k + 1], (sublanes, lanes))
            spot = place_of[k, j] + sublane
            for i in range(groups):
                hit = jnp.logical_and(column == names[i], spot < places[i])
                found[i] = jnp.maximum(found[i], jnp.where(hit, spot, 0))
            hit = column == r * cheight + lane
            found[groups] = jnp.maximum(found[groups], jnp.where(hit, spot, 0))
    for i in range(groups + 1):
        best = found[i]
        for shift in (1, 2, 4):
            best = jnp.maximum(best, pltpu.roll(best, shift, 0))
        tables[pl.ds(sublanes * i, sublanes)] = best
    to_scalar = load(tables, chain, 7)
    to_scalar.start()
    sums[0] = jnp.zeros(sums.shape[1:], f32)
    to_scalar.wait()
    later_loads[0].wait()
    later_loads[1].wait()

    base = flat * height - margin

    def residual_low(i):
        residual = rhs[i] - row_product(i, fine_cols, i, base, blocks, diag, ext1, margin + i)
        ext2[margin + i] = residual.astype(low)

    def second(i):
        value = iterate[i] + damping * dot(smoother[i], ext2[margin + i])
        iterate[i] = value
        ext2[margin + i] = value.astype(low)

    for j in range(steps):
        push(min(2 * j + 2 + depth, second_queue))
        wait_halo(0, j)
        for body in (residual_low, second):
            rows(margin - (j + 1) * chunk, chunk, body, 4)
            rows(margin + j * chunk, chunk, body, 4)
    push(second_queue + depth)

    def third(shift):
        def body(i):
            residual = rhs[i] - row_product(i, fine_cols, i, base, blocks, diag, ext2, margin + i)
            own_full[i + shift] = residual
            own_low[i + shift] = residual.astype(low)

        return body

    def near(j, count=sublanes):
        at = pl.ds(j * sublanes, count)
        return remote(own_full.at[at], near_full.at[at], near_send.at[0], near_recv.at[j], partner)

    def far(o, begin, count, j=0):
        at = pl.ds(begin, count)
        return remote(own_low.at[at], far_low.at[o - 1, at], far_send.at[o - 1], far_recv.at[o - 1, j], peer(o, True))

    def via(o, j, count=sublanes):
        at = pl.ds(j * sublanes, count)
        return remote(
            far_low.at[o - 1, at], via_low.at[o - 1, at], via_send.at[o - 1], via_recv.at[o - 1, j], partner
        )

    def absorb(k, j):
        source = (own_full, near_full)[k] if k < 2 else (via_low if k % 2 else far_low).at[k // 2 - 1]
        spot = place_of[k, j] - j * sublanes

        def body(at):
            sums[at + spot] = source[at].astype(f32) + sums[chain[sublanes * k, at]]

        rows(j * sublanes, sublanes, body, 4)

    for k, j in order:
        o = k // 2
        if k == 0:
            push(second_queue + 2 * j + 2 + depth)
            wait_halo(1, j)
            for n in (0, 1):
                start, at = starts[2 * j + n], (2 * j + n) * chunk
                rows(start, chunk, third(at - start), 4)
                for o in range(1, chips):
                    far(o, at, chunk, j).start()
            near(j).start()
            absorb(k, j)
        elif k == 1:
            near(j).wait_recv()
            absorb(k, j)
        elif k % 2 == 0:
            far(o, j * sublanes, sublanes, j).wait_recv()
            via(o, j).start()
            absorb(k, j)
        else:
            via(o, j).wait_recv()
            absorb(k, j)
    for c in later_loads[2:]:
        c.wait()

    def coarse_first(c):
        value = damping * dot(csmoother[c], sums[chain[sublanes * groups, c]].astype(low))
        cfirst[c] = value
        cext[cmargin + c] = value.astype(low)

    def spot_of(u):
        return side * (cmargin - (u + 1) * csub) + core * u * csub

    def across(p):
        at = spot_of(p * chips + chip)
        src = cext.at[pl.ds(cmargin + side * cmargin + at, csub)]
        return remote(src, clanding.at[pl.ds(at, csub)], cx_send.at[0], cx_recv.at[p], forth)

    def forward(o, p):
        at = pl.ds(spot_of(p * chips + chip), csub)
        return remote(clanding.at[at], clanding.at[at], cf_send.at[o - 1], cf_recv.at[o - 1, p], peer(o, True))

    for p in range(parts):
        rows(side * cmargin + spot_of(p * chips + chip), csub, coarse_first, csub)
        pl.when(can_send)(lambda: across(p).start())
    for p in range(parts):
        for o in range(1, chips):
            rows(side * cmargin + spot_of(p * chips + (chip + o) % chips), csub, coarse_first, csub)
    rows(core * cmargin, cmargin, coarse_first, 4)

    cbase = r * cheight - cmargin
    own = core * cmargin

    def coarse_residual(n):
        image = row_product(n, coarse_cols, own + n, cbase, cblocks, cdiag, cext, cmargin + own + n)
        cres[n] = (sums[chain[sublanes * groups, own + n]] - image).astype(low)

    def coarse_second(n):
        correction[own + n] = cfirst[own + n] + damping * dot(csmoother[own + n], cres[n])

    def back(p):
        at = pl.ds(own + side * (cmargin - (p + 1) * span) + core * p * span, span)
        return remote(correction.at[at], correction.at[at], cp_sem.at[0], cp_sem.at[1], partner)

    halves = correction.at[mine]
    all_back = remote(halves, halves, cp_sem.at[0], cp_sem.at[1], partner)
    sent = clanding.at[pl.ds(0, parts * csub)]
    all_across = remote(sent, sent, cx_send.at[0], cx_recv.at[0], forth)
    all_forward = [remote(sent, sent, cf_send.at[o - 1], cf_recv.at[o - 1, 0], peer(o, True)) for o in range(1, chips)]

    def receive(p):
        def go():
            across(p).wait_recv()
            for o in range(1, chips):
                forward(o, p).start()

        pl.when(can_recv)(go)

    for p in range(parts):
        receive(p)
    for p in range(parts):
        begin = side * (cmargin - (p + 1) * span) + core * p * span

        def arrived():
            for o in range(1, chips):
                forward(o, p).wait_recv()

            def place(n):
                cext[core * (cmargin + cheight) + n] = clanding[n]

            rows(begin, span, place, span)

        pl.when(can_recv)(arrived)
        rows(begin, span, coarse_residual, 4)
        rows(begin, span, coarse_second, 4)
        back(p).start()
    all_back.wait_recv()

    cstart = r * cheight

    def final(i):
        iterate[i] = iterate[i] + correction[jnp.clip(aggregate[i] - cstart, 0, cheight - 1)]

    rows(0, height, final, 4)

    for n in range(len(queue) - depth, len(queue)):
        wait_sent(n)
    all_names.wait_send()
    near(0, height).wait_send()
    for o in range(1, chips):
        far(o, 0, height).wait_send()
        via(o, 0, height).wait_send()

    for c in all_forward:
        pl.when(can_recv)(lambda: c.wait_send())
    pl.when(can_send)(lambda: all_across.wait_send())
    all_back.wait_send()


def on_device(
    groups, ranks,
    rhs, fine_diag, fine_smoother, fine_blocks, fine_cols, aggregate,
    coarse_diag, coarse_smoother, coarse_blocks, coarse_cols,
):
    height, b, n = rhs.shape
    cheight = coarse_diag.shape[0]
    cmargin = cheight // 2
    neighbours = fine_blocks.shape[1]
    chips = groups // 2
    steps = height // sublanes
    parts = cmargin // (csub * chips)
    vmem = pltpu.VMEM
    dma = pltpu.SemaphoreType.DMA
    smem = pl.BlockSpec(memory_space=pltpu.SMEM)
    hbm = pl.BlockSpec(memory_space=pl.ANY)
    return pl.pallas_call(
        functools.partial(kernel, groups, ranks),
        out_shape=pltpu.VMEM(rhs.shape, f32),
        in_specs=[smem] * 3 + [hbm] * 7,
        out_specs=pl.BlockSpec(memory_space=pltpu.VMEM),
        scratch_shapes=[
            vmem((height, b, n), f32),
            vmem((height, b, b), low),
            vmem((height, b, b), low),
            vmem((height, neighbours, b, b), low),
            vmem((cmargin, b, b), low),
            vmem((cheight, b, b), low),
            vmem((cmargin, neighbours, b, b), low),
            vmem((2 * height, b, n), low),
            vmem((2 * height, b, n), low),
            vmem((2, height // 2, b, n), low),
            vmem((2, height // 2, b, n), low),
            vmem((height, b, n), f32),
            vmem((height, b, n), low),
            vmem((height, b, n), f32),
            vmem((chips - 1, height, b, n), low),
            vmem((chips - 1, height, b, n), low),
            vmem((groups * height + 1, b, n), f32),
            vmem((groups, sublanes, lanes), jnp.int32),
            vmem(((groups + 1) * sublanes, lanes), jnp.int32),
            pltpu.SMEM(((groups + 1) * sublanes, lanes), jnp.int32),
            vmem((cheight, b, n), f32),
            vmem((cmargin, b, n), low),
            vmem((2 * cheight, b, n), low),
            vmem((cmargin, b, n), low),
            vmem((cheight, b, n), f32),
            dma((8,)),
            dma((2, depth)),
            dma((2, 2, steps)),
            dma((2,)),
            dma((1,)),
            dma((steps,)),
            dma((chips - 1,)),
            dma((chips - 1, steps)),
            dma((chips - 1,)),
            dma((chips - 1, steps)),
            dma((1,)),
            dma((parts,)),
            dma((chips - 1,)),
            dma((chips - 1, parts)),
            dma((2,)),
        ],
        compiler_params=pltpu.CompilerParams(
            collective_id=0, has_side_effects=True, vmem_limit_bytes=58 * 1024 * 1024
        ),
        name="cycle",
    )(
        fine_cols.T, coarse_cols.T, aggregate,
        rhs, fine_diag, fine_smoother, fine_blocks, coarse_diag, coarse_smoother, coarse_blocks,
    )


def solution(mesh):
    fine = P(("grp", "rows"))
    return jax.shard_map(
        functools.partial(on_device, mesh.shape["grp"], mesh.shape["rows"]),
        mesh=mesh,
        in_specs=(fine,) * 6 + (P("rows"),) * 4,
        out_specs=fine,
        check_vma=False,
    )
```

```python
import functools

import jax
import jax.numpy as jnp
from jax import lax
from jax.experimental import pallas as pl
from jax.experimental.pallas import tpu as pltpu
from jax.sharding import PartitionSpec as P

MESH = pl.DeviceIdType.MESH
damping = 0.8
lanes = 128
sublanes = 8
depth = 4
fewer = 3
later = 3
early = 8
csub = 2
low = jnp.bfloat16
f32 = jnp.float32


def dot(a, b):
    return jnp.dot(a, b, preferred_element_type=f32)


def row_product(i, columns, at, base, offs, diag, extended, own):
    count = offs.shape[1]
    last = extended.shape[0] - 1
    vectors = [extended[jnp.clip(columns[k, at] - base, 0, last)] for k in range(count)] + [extended[own]]
    blocks = [offs[i, k] for k in range(count)] + [diag[i]]
    total = None
    for p in range(0, count + 1, 4):
        term = dot(
            jnp.concatenate(blocks[p : p + 4], axis=1),
            jnp.concatenate(vectors[p : p + 4], axis=0),
        )
        total = term if total is None else total + term
    return total


def absorb_order(steps):
    order = [(k, t - k) for t in range(steps + 1) for k in (0, 1)]
    return [(k, j) for k, j in order if 0 <= j < steps]


def kernel(
    groups, ranks,
    fine_cols, coarse_cols, aggregate,
    rhs_hbm, diag_hbm, smoother_hbm, blocks_hbm, cdiag_hbm, csmoother_hbm, cblocks_hbm,
    iterate,
    rhs, diag, smoother, blocks, cdiag, csmoother, cblocks,
    ext1, ext2, landing1, landing2,
    own_full, near_full, sums, names, tables, chain,
    half_out, half_in, crhs, cfirst, cres, cext, clanding, correction,
    load_sem, halo_send, halo_recv, name_sem, near_send, near_recv,
    half_send, half_recv, cx_send, cx_recv, mate_sem, cp_sem,
):
    g = lax.axis_index("grp")
    r = lax.axis_index("rows")
    height = rhs.shape[0]
    margin = height // 2
    steps = height // sublanes
    chunk = sublanes // 2
    piece = chunk // 2
    cheight = correction.shape[0]
    cmargin = cheight // 2
    chips = groups // 2
    parts = cmargin // csub
    group = sublanes // csub

    flat = g * ranks + r
    has_left = flat > 0
    has_right = flat < groups * ranks - 1
    left = ((flat - 1) // ranks, (flat + ranks - 1) % ranks)
    right = ((flat + 1) // ranks, (flat + 1) % ranks)
    core = g % 2
    chip = g // 2
    partner = (chip * 2 + 1 - core, r)
    side = 1 - core
    forth = (chip * 2 + 1 - core, r - 1 + 2 * core)
    linked = jnp.where(core == 0, r > 0, r < ranks - 1)

    def peer(o):
        return (((chip + o) % chips) * 2 + core, r)

    def load(src, dst, at):
        return pltpu.make_async_copy(src, dst, load_sem.at[at])

    mine = pl.ds(core * cmargin, cmargin)
    first_loads = [load(rhs_hbm, rhs, 0), load(smoother_hbm, smoother, 1)]
    later_loads = [
        load(blocks_hbm, blocks, 2),
        load(diag_hbm, diag, 3),
        load(csmoother_hbm.at[mine], csmoother, 4),
        load(cdiag_hbm.at[mine], cdiag, 5),
        load(cblocks_hbm.at[mine], cblocks, 6),
    ]
    for c in first_loads:
        c.start()

    barrier = pltpu.get_barrier_semaphore()

    def greet(device):
        pl.semaphore_signal(barrier, inc=1, device_id=device, device_id_type=MESH)

    pl.when(has_left)(lambda: greet(left))
    pl.when(has_right)(lambda: greet(right))
    greet(partner)
    pl.when(linked)(lambda: greet(forth))
    for o in range(1, chips):
        greet(peer(o))
    met = chips + has_left.astype(jnp.int32) + has_right.astype(jnp.int32) + linked.astype(jnp.int32)

    def remote(src, dst, send, recv, device):
        return pltpu.make_async_remote_copy(
            src_ref=src, dst_ref=dst, send_sem=send, recv_sem=recv, device_id=device, device_id_type=MESH
        )

    pieces = margin // piece
    queue = [(0, j * piece, piece) for j in range(pieces)] + [(1, margin - piece, piece)]
    queue += [(1, j * piece, piece) for j in range(pieces - 1)]
    second_queue = pieces + 1
    pushed, drained = [], []
    exts, landings = (ext1, ext2), (landing1, landing2)

    def to_right(n, item=None):
        phase, start, count = item or queue[n]
        src = exts[phase].at[pl.ds(margin + height - start - count, count)]
        dst = landings[phase].at[0, pl.ds(margin - start - count, count)]
        return remote(src, dst, halo_send.at[0, n % depth], halo_recv.at[phase, 0, start // chunk], right)

    def to_left(n, item=None):
        phase, start, count = item or queue[n]
        src = exts[phase].at[pl.ds(margin + start, count)]
        dst = landings[phase].at[1, pl.ds(start, count)]
        return remote(src, dst, halo_send.at[1, n % depth], halo_recv.at[phase, 1, start // chunk], left)

    def wait_sent(n):
        pl.when(has_right)(lambda: to_right(n).wait_send())
        pl.when(has_left)(lambda: to_left(n).wait_send())

    def launch(n):
        if n < second_queue:
            window = depth
        else:
            window = fewer if n < second_queue + 4 else later
        while len(drained) <= n - window:
            wait_sent(len(drained))
            drained.append(None)
        pl.when(has_right)(lambda: to_right(n).start())
        pl.when(has_left)(lambda: to_left(n).start())

    def push(upto):
        while len(pushed) < min(upto, len(queue)):
            launch(len(pushed))
            pushed.append(None)

    def rows(start, count, body, unroll):
        def step(n, carry):
            body(start + n)
            return carry

        lax.fori_loop(0, count, step, 0, unroll=unroll)

    def wait_halo(phase, j):
        start, count = j * chunk, chunk
        pl.when(has_left)(lambda: to_right(0, (phase, start, count)).wait_recv())
        pl.when(has_right)(lambda: to_left(0, (phase, start, count)).wait_recv())
        ext, landing = exts[phase], landings[phase]

        def place_low(i):
            ext[i] = landing[0, i]

        def place_high(i):
            ext[margin + height + i] = landing[1, i]

        pl.when(has_left)(lambda: rows(margin - start - count, count, place_low, count))
        pl.when(has_right)(lambda: rows(start, count, place_high, count))

    starts = [at for j in range(steps) for at in (margin - (j + 1) * chunk, margin + j * chunk)]

    lane = lax.broadcasted_iota(jnp.int32, (sublanes, lanes), 1)
    sublane = lax.broadcasted_iota(jnp.int32, (sublanes, lanes), 0)
    named = jnp.zeros((sublanes, lanes), jnp.int32)
    for n, start in enumerate(starts):
        for m in range(chunk):
            named = jnp.where(lane == n * chunk + m, aggregate[start + m], named)
    names[0] = named

    name_copy = remote(names.at[0], names.at[1], name_sem.at[0], name_sem.at[1], partner)

    for c in first_loads:
        c.wait()
    for c in later_loads:
        c.start()

    def first(i):
        value = damping * dot(smoother[i], rhs[i].astype(low))
        iterate[i] = value
        ext1[margin + i] = value.astype(low)

    for j in range(steps):
        rows(height - (j + 1) * chunk, chunk, first, 4)
        rows(j * chunk, chunk, first, 4)
        if j == 1:
            pl.semaphore_wait(barrier, met)
            push(depth)
            name_copy.start()

    order = absorb_order(steps)
    place_of = {key: 1 + sublanes * n for n, key in enumerate(order)}
    name_copy.wait_recv()
    columns = jnp.zeros((sublanes, lanes), jnp.int32)
    places = []
    for k in (0, 1):
        columns = jnp.where(sublane == k, names[k], columns)
        spot = lane % sublanes
        for j in range(steps):
            spot = jnp.where(lane // sublanes == j, spot + place_of[k, j], spot)
        places.append(spot)
    columns = columns.T
    found = [jnp.zeros((sublanes, lanes), jnp.int32) for _ in range(3)]
    for k in (0, 1):
        for j in range(steps):
            column = jnp.broadcast_to(columns[sublanes * j : sublanes * (j + 1), k : k + 1], (sublanes, lanes))
            spot = place_of[k, j] + sublane
            for i in (0, 1):
                hit = jnp.logical_and(column == names[i], spot < places[i])
                found[i] = jnp.maximum(found[i], jnp.where(hit, spot, 0))
            hit = column == r * cheight + lane
            found[2] = jnp.maximum(found[2], jnp.where(hit, spot, 0))
    for i in range(3):
        best = found[i]
        for shift in (1, 2, 4):
            best = jnp.maximum(best, pltpu.roll(best, shift, 0))
        tables[pl.ds(sublanes * i, sublanes)] = best
    to_scalar = load(tables, chain, 7)
    to_scalar.start()
    sums[0] = jnp.zeros(sums.shape[1:], f32)
    to_scalar.wait()
    later_loads[0].wait()
    later_loads[1].wait()

    base = flat * height - margin

    def residual_low(i):
        residual = rhs[i] - row_product(i, fine_cols, i, base, blocks, diag, ext1, margin + i)
        ext2[margin + i] = residual.astype(low)

    def second(i):
        value = iterate[i] + damping * dot(smoother[i], ext2[margin + i])
        iterate[i] = value
        ext2[margin + i] = value.astype(low)

    for j in range(steps):
        push(min(2 * j + 2 + depth, second_queue))
        wait_halo(0, j)
        for body in (residual_low, second):
            for n in range(sublanes):
                body(starts[2 * j + n // chunk] + n % chunk)
    push(second_queue + 2)

    def third(i, at):
        residual = rhs[i] - row_product(i, fine_cols, i, base, blocks, diag, ext2, margin + i)
        own_full[at] = residual

    def near(j, count=sublanes):
        at = pl.ds(j * sublanes, count)
        return remote(own_full.at[at], near_full.at[at], near_send.at[0], near_recv.at[j], partner)

    def absorb(k, j):
        source = (own_full, near_full)[k]
        spot = place_of[k, j] - j * sublanes

        def body(at):
            sums[at + spot] = source[at] + sums[chain[sublanes * k, at]]

        rows(j * sublanes, sublanes, body, 4)

    for k, j in order:
        if k == 0:
            push(second_queue + 2 * j + 2 + later)
            wait_halo(1, j)
            for n in range(sublanes):
                third(starts[2 * j + n // chunk] + n % chunk, j * sublanes + n)
            near(j).start()
        else:
            near(j).wait_recv()
        absorb(k, j)

    own = core * cmargin

    def whole(n):
        return sums[chain[2 * sublanes, own + n]]

    def begin(p):
        return core * (cmargin - (p + 1) * csub) + side * p * csub

    def half(o, p, count=csub):
        at = pl.ds(p * csub, count)
        return remote(half_out.at[at], half_in.at[o - 1, at], half_send.at[o - 1], half_recv.at[o - 1, p], peer(o))

    def share(p):
        for n in range(csub):
            half_out[p * csub + n] = whole(begin(p) + n).astype(low)
        for o in range(1, chips):
            half(o, p).start()

    for p in range(early):
        share(p)
    for c in later_loads[2:]:
        c.wait()

    def across(p):
        src = cext.at[pl.ds(cmargin + own + begin(p), csub)]
        return remote(src, clanding.at[pl.ds(begin(p), csub)], cx_send.at[0], cx_recv.at[p], forth)

    def mate(p):
        at = pl.ds(cmargin + own + begin(p), csub)
        return remote(cext.at[at], cext.at[at], mate_sem.at[0], mate_sem.at[1], partner)

    for p in range(parts):
        if p + early < parts:
            share(p + early)
        for o in range(1, chips):
            half(o, p).wait_recv()
        for m in range(csub):
            n = begin(p) + m
            total = whole(n)
            for o in range(1, chips):
                total = total + half_in[o - 1, p * csub + m].astype(f32)
            crhs[n] = total
            value = damping * dot(csmoother[n], total.astype(low))
            cfirst[n] = value
            cext[cmargin + own + n] = value.astype(low)
        pl.when(linked)(lambda: across(p).start())
        mate(p).start()

    cbase = r * cheight - cmargin

    def coarse_residual(n):
        image = row_product(n, coarse_cols, own + n, cbase, cblocks, cdiag, cext, cmargin + own + n)
        cres[n] = (crhs[n] - image).astype(low)

    def coarse_second(n):
        correction[own + n] = cfirst[n] + damping * dot(csmoother[n], cres[n])

    def back(k):
        at = pl.ds(own + side * (cmargin - (k + 1) * sublanes) + core * k * sublanes, sublanes)
        return remote(correction.at[at], correction.at[at], cp_sem.at[0], cp_sem.at[1], partner)

    halves = correction.at[mine]
    all_back = remote(halves, halves, cp_sem.at[0], cp_sem.at[1], partner)
    all_mate = remote(clanding, clanding, mate_sem.at[0], mate_sem.at[1], partner)
    all_across = remote(clanding, clanding, cx_send.at[0], cx_recv.at[0], forth)
    all_mate.wait_recv()
    for k in range(parts // group):
        first_row = side * (cmargin - (k + 1) * sublanes) + core * k * sublanes

        def arrived():
            for p in range(k * group, (k + 1) * group):
                across(p).wait_recv()

            def place(n):
                cext[core * (cmargin + cheight) + n] = clanding[n]

            rows(first_row, sublanes, place, 4)

        pl.when(linked)(arrived)
        for body in (coarse_residual, coarse_second):
            for n in range(sublanes):
                body(first_row + n)
        back(k).start()
    all_back.wait_recv()

    cstart = r * cheight

    def final(i):
        iterate[i] = iterate[i] + correction[jnp.clip(aggregate[i] - cstart, 0, cheight - 1)]

    rows(0, height, final, 4)

    for n in range(len(drained), len(queue)):
        wait_sent(n)
    name_copy.wait_send()
    near(0, height).wait_send()
    for o in range(1, chips):
        half(o, 0, cmargin).wait_send()

    pl.when(linked)(lambda: all_across.wait_send())
    all_mate.wait_send()
    all_back.wait_send()


def on_device(
    groups, ranks,
    rhs, fine_diag, fine_smoother, fine_blocks, fine_cols, aggregate,
    coarse_diag, coarse_smoother, coarse_blocks, coarse_cols,
):
    height, b, n = rhs.shape
    cheight = coarse_diag.shape[0]
    cmargin = cheight // 2
    neighbours = fine_blocks.shape[1]
    chips = groups // 2
    steps = height // sublanes
    parts = cmargin // csub
    vmem = pltpu.VMEM
    dma = pltpu.SemaphoreType.DMA
    smem = pl.BlockSpec(memory_space=pltpu.SMEM)
    hbm = pl.BlockSpec(memory_space=pl.ANY)
    return pl.pallas_call(
        functools.partial(kernel, groups, ranks),
        out_shape=pltpu.VMEM(rhs.shape, f32),
        in_specs=[smem] * 3 + [hbm] * 7,
        out_specs=pl.BlockSpec(memory_space=pltpu.VMEM),
        scratch_shapes=[
            vmem((height, b, n), f32),
            vmem((height, b, b), low),
            vmem((height, b, b), low),
            vmem((height, neighbours, b, b), low),
            vmem((cmargin, b, b), low),
            vmem((cmargin, b, b), low),
            vmem((cmargin, neighbours, b, b), low),
            vmem((2 * height, b, n), low),
            vmem((2 * height, b, n), low),
            vmem((2, height // 2, b, n), low),
            vmem((2, height // 2, b, n), low),
            vmem((height, b, n), f32),
            vmem((height, b, n), f32),
            vmem((2 * height + 1, b, n), f32),
            vmem((2, sublanes, lanes), jnp.int32),
            vmem((3 * sublanes, lanes), jnp.int32),
            pltpu.SMEM((3 * sublanes, lanes), jnp.int32),
            vmem((cmargin, b, n), low),
            vmem((chips - 1, cmargin, b, n), low),
            vmem((cmargin, b, n), f32),
            vmem((cmargin, b, n), f32),
            vmem((cmargin, b, n), low),
            vmem((2 * cheight, b, n), low),
            vmem((cmargin, b, n), low),
            vmem((cheight, b, n), f32),
            dma((8,)),
            dma((2, depth)),
            dma((2, 2, steps)),
            dma((2,)),
            dma((1,)),
            dma((steps,)),
            dma((chips - 1,)),
            dma((chips - 1, parts)),
            dma((1,)),
            dma((parts,)),
            dma((2,)),
            dma((2,)),
        ],
        compiler_params=pltpu.CompilerParams(
            collective_id=0, has_side_effects=True, vmem_limit_bytes=58 * 1024 * 1024
        ),
        name="cycle",
    )(
        fine_cols.T, coarse_cols.T, aggregate,
        rhs, fine_diag, fine_smoother, fine_blocks, coarse_diag, coarse_smoother, coarse_blocks,
    )


def solution(mesh):
    fine = P(("grp", "rows"))
    return jax.shard_map(
        functools.partial(on_device, mesh.shape["grp"], mesh.shape["rows"]),
        mesh=mesh,
        in_specs=(fine,) * 6 + (P("rows"),) * 4,
        out_specs=fine,
        check_vma=False,
    )
```

```python
import functools

import jax
import jax.numpy as jnp
from jax import lax
from jax.experimental import pallas as pl
from jax.experimental.pallas import tpu as pltpu
from jax.sharding import PartitionSpec as P

MESH = pl.DeviceIdType.MESH
damping = 0.8
lanes = 128
sublanes = 8
depth = 8
fewer = 3
later = 4
early = 8
csub = 2
low = jnp.bfloat16
f32 = jnp.float32


def dot(a, b):
    return jnp.dot(a, b, preferred_element_type=f32)


def pack(i, offs, diag, packed):
    packed[i] = jnp.concatenate([offs[i, k] for k in range(offs.shape[1])] + [diag[i]], axis=1)


def row_product(i, columns, at, base, packed, extended, own):
    count = columns.shape[0]
    width = packed.shape[2] // (count + 1)
    last = extended.shape[0] - 1
    vectors = [extended[jnp.clip(columns[k, at] - base, 0, last)] for k in range(count)] + [extended[own]]
    total = None
    for p in range(0, count + 1, 4):
        group = vectors[p : p + 4]
        term = dot(packed[i, :, width * p : width * (p + len(group))], jnp.concatenate(group, axis=0))
        total = term if total is None else total + term
    return total


def absorb_order(steps):
    order = [(k, t - k) for t in range(steps + 1) for k in (0, 1)]
    return [(k, j) for k, j in order if 0 <= j < steps]


def kernel(
    groups, ranks,
    fine_cols, coarse_cols, aggregate,
    rhs_hbm, diag_hbm, smoother_hbm, blocks_hbm, cdiag_hbm, csmoother_hbm, cblocks_hbm,
    iterate,
    rhs, diag, smoother, blocks, cdiag, csmoother, cblocks, packed, cpacked,
    ext1, ext2, landing1, landing2,
    own_full, near_full, sums, names, tables, chain,
    half_out, half_in, crhs, cfirst, cres, cext, clanding, correction,
    load_sem, halo_send, halo_recv, name_sem, near_send, near_recv,
    half_send, half_recv, cx_send, cx_recv, mate_sem, cp_sem,
):
    g = lax.axis_index("grp")
    r = lax.axis_index("rows")
    height = rhs.shape[0]
    margin = height // 2
    steps = height // sublanes
    chunk = sublanes // 2
    piece = chunk // 2
    cheight = correction.shape[0]
    cmargin = cheight // 2
    chips = groups // 2
    parts = cmargin // csub
    group = sublanes // csub

    flat = g * ranks + r
    has_left = flat > 0
    has_right = flat < groups * ranks - 1
    left = ((flat - 1) // ranks, (flat + ranks - 1) % ranks)
    right = ((flat + 1) // ranks, (flat + 1) % ranks)
    core = g % 2
    chip = g // 2
    partner = (chip * 2 + 1 - core, r)
    side = 1 - core
    forth = (chip * 2 + 1 - core, r - 1 + 2 * core)
    linked = jnp.where(core == 0, r > 0, r < ranks - 1)

    def peer(o):
        return (((chip + o) % chips) * 2 + core, r)

    def load(src, dst, at):
        return pltpu.make_async_copy(src, dst, load_sem.at[at])

    mine = pl.ds(core * cmargin, cmargin)
    edge = sublanes
    pairs = [(rhs_hbm, rhs), (smoother_hbm, smoother)]
    spans = [pl.ds(0, edge), pl.ds(height - edge, edge), pl.ds(edge, height - 2 * edge)]
    edge_loads = [load(a.at[at], b.at[at], 8 + 2 * n + m) for n, at in enumerate(spans[:2]) for m, (a, b) in enumerate(pairs)]
    first_loads = [load(a.at[spans[2]], b.at[spans[2]], m) for m, (a, b) in enumerate(pairs)]
    later_loads = [
        load(blocks_hbm, blocks, 2),
        load(diag_hbm, diag, 3),
        load(csmoother_hbm.at[mine], csmoother, 4),
        load(cdiag_hbm.at[mine], cdiag, 5),
        load(cblocks_hbm.at[mine], cblocks, 6),
    ]
    for c in edge_loads + first_loads:
        c.start()

    barrier = pltpu.get_barrier_semaphore()

    def greet(device):
        pl.semaphore_signal(barrier, inc=1, device_id=device, device_id_type=MESH)

    pl.when(has_left)(lambda: greet(left))
    pl.when(has_right)(lambda: greet(right))
    greet(partner)
    pl.when(linked)(lambda: greet(forth))
    for o in range(1, chips):
        greet(peer(o))
    met = chips + has_left.astype(jnp.int32) + has_right.astype(jnp.int32) + linked.astype(jnp.int32)

    def remote(src, dst, send, recv, device):
        return pltpu.make_async_remote_copy(
            src_ref=src, dst_ref=dst, send_sem=send, recv_sem=recv, device_id=device, device_id_type=MESH
        )

    pieces = margin // piece
    queue = [(0, j * piece, piece) for j in range(pieces)] + [(1, margin - piece, piece)]
    queue += [(1, j * piece, piece) for j in range(pieces - 1)]
    second_queue = pieces + 1
    pushed, drained = [], []
    exts, landings = (ext1, ext2), (landing1, landing2)

    def to_right(n, item=None):
        phase, start, count = item or queue[n]
        src = exts[phase].at[pl.ds(margin + height - start - count, count)]
        dst = landings[phase].at[0, pl.ds(margin - start - count, count)]
        return remote(src, dst, halo_send.at[0, n % depth], halo_recv.at[phase, start // chunk], right)

    def to_left(n, item=None):
        phase, start, count = item or queue[n]
        src = exts[phase].at[pl.ds(margin + start, count)]
        dst = landings[phase].at[1, pl.ds(start, count)]
        return remote(src, dst, halo_send.at[1, n % depth], halo_recv.at[phase, start // chunk], left)

    def wait_sent(n):
        pl.when(has_right)(lambda: to_right(n).wait_send())
        pl.when(has_left)(lambda: to_left(n).wait_send())

    def launch(n):
        if n < second_queue:
            window = depth
        else:
            window = fewer if n < second_queue + 4 else later
        while len(drained) <= n - window:
            wait_sent(len(drained))
            drained.append(None)
        pl.when(has_right)(lambda: to_right(n).start())
        pl.when(has_left)(lambda: to_left(n).start())

    def push(upto):
        while len(pushed) < min(upto, len(queue)):
            launch(len(pushed))
            pushed.append(None)

    def rows(start, count, body, unroll):
        def step(n, carry):
            body(start + n)
            return carry

        lax.fori_loop(0, count, step, 0, unroll=unroll)

    def wait_halo(phase, j):
        start, count = j * chunk, chunk
        ext, landing = exts[phase], landings[phase]
        sides = landing.at[:, pl.ds(start, count)]
        both = remote(sides, sides, halo_send.at[0, 0], halo_recv.at[phase, j], left)
        pl.when(jnp.logical_and(has_left, has_right))(lambda: both.wait_recv())
        pl.when(jnp.logical_not(has_right))(lambda: to_right(0, (phase, start, count)).wait_recv())
        pl.when(jnp.logical_not(has_left))(lambda: to_left(0, (phase, start, count)).wait_recv())

        def place_low(i):
            ext[i] = landing[0, i]

        def place_high(i):
            ext[margin + height + i] = landing[1, i]

        pl.when(has_left)(lambda: rows(margin - start - count, count, place_low, count))
        pl.when(has_right)(lambda: rows(start, count, place_high, count))

    starts = [at for j in range(steps) for at in (margin - (j + 1) * chunk, margin + j * chunk)]

    lane = lax.broadcasted_iota(jnp.int32, (sublanes, lanes), 1)
    sublane = lax.broadcasted_iota(jnp.int32, (sublanes, lanes), 0)
    named = jnp.zeros((sublanes, lanes), jnp.int32)
    for n, start in enumerate(starts):
        for m in range(chunk):
            named = jnp.where(lane == n * chunk + m, aggregate[start + m], named)
    names[0] = named

    name_copy = remote(names.at[0], names.at[1], name_sem.at[0], name_sem.at[1], partner)

    for c in edge_loads:
        c.wait()

    def first(i):
        value = damping * dot(smoother[i], rhs[i].astype(low))
        iterate[i] = value
        ext1[margin + i] = value.astype(low)

    for j in range(steps):
        rows(height - (j + 1) * chunk, chunk, first, 4)
        rows(j * chunk, chunk, first, 4)
        if j == 1:
            pl.semaphore_wait(barrier, met)
            push(2 * j + 2)
            for c in first_loads:
                c.wait()
            for c in later_loads:
                c.start()

        elif 1 < j and 2 * j + 2 <= depth:
            push(2 * j + 2)
    name_copy.start()
    order = absorb_order(steps)
    place_of = {key: 1 + sublanes * n for n, key in enumerate(order)}
    name_copy.wait_recv()
    columns = jnp.zeros((sublanes, lanes), jnp.int32)
    places = []
    for k in (0, 1):
        columns = jnp.where(sublane == k, names[k], columns)
        spot = lane % sublanes
        for j in range(steps):
            spot = jnp.where(lane // sublanes == j, spot + place_of[k, j], spot)
        places.append(spot)
    columns = columns.T
    found = [jnp.zeros((sublanes, lanes), jnp.int32) for _ in range(3)]
    for k in (0, 1):
        for j in range(steps):
            column = jnp.broadcast_to(columns[sublanes * j : sublanes * (j + 1), k : k + 1], (sublanes, lanes))
            spot = place_of[k, j] + sublane
            for i in (0, 1):
                hit = jnp.logical_and(column == names[i], spot < places[i])
                found[i] = jnp.maximum(found[i], jnp.where(hit, spot, 0))
            hit = column == r * cheight + lane
            found[2] = jnp.maximum(found[2], jnp.where(hit, spot, 0))
    for i in range(3):
        best = found[i]
        for shift in (1, 2, 4):
            best = jnp.maximum(best, pltpu.roll(best, shift, 0))
        tables[pl.ds(sublanes * i, sublanes)] = best
    to_scalar = load(tables, chain, 7)
    to_scalar.start()
    sums[0] = jnp.zeros(sums.shape[1:], f32)
    to_scalar.wait()
    later_loads[0].wait()
    later_loads[1].wait()

    base = flat * height - margin

    def residual_low(i):
        residual = rhs[i] - row_product(i, fine_cols, i, base, packed, ext1, margin + i)
        ext2[margin + i] = residual.astype(low)

    def second(i):
        value = iterate[i] + damping * dot(smoother[i], ext2[margin + i])
        iterate[i] = value
        ext2[margin + i] = value.astype(low)

    def pack_step(j):
        for start in starts[2 * j : 2 * j + 2]:
            rows(start, chunk, lambda i: pack(i, blocks, diag, packed), 2)

    pack_step(0)
    pack_step(1)
    for j in range(steps):
        push(min(2 * j + 2 + depth, second_queue))
        if j + 2 < steps:
            pack_step(j + 2)
        if j == 1:
            for c in later_loads[2:]:
                c.wait()
        if 1 <= j < 5:
            share_rows = cmargin // 4
            rows((j - 1) * share_rows, share_rows, lambda i: pack(i, cblocks, cdiag, cpacked), 2)
        wait_halo(0, j)
        for body in (residual_low, second):
            for n in range(sublanes):
                body(starts[2 * j + n // chunk] + n % chunk)
    push(second_queue + 2)

    def third(i, at):
        residual = rhs[i] - row_product(i, fine_cols, i, base, packed, ext2, margin + i)
        own_full[at] = residual

    def near(j, count=sublanes):
        at = pl.ds(j * sublanes, count)
        return remote(own_full.at[at], near_full.at[at], near_send.at[0], near_recv.at[j], partner)

    def absorb(k, j):
        source = (own_full, near_full)[k]
        spot = place_of[k, j] - j * sublanes

        def body(at):
            sums[at + spot] = source[at] + sums[chain[sublanes * k, at]]

        rows(j * sublanes, sublanes, body, 4)

    for k, j in order:
        if k == 0:
            push(second_queue + 2 * j + 2 + later)
            wait_halo(1, j)
            for n in range(sublanes):
                third(starts[2 * j + n // chunk] + n % chunk, j * sublanes + n)
            near(j).start()
        else:
            near(j).wait_recv()
        absorb(k, j)

    own = core * cmargin

    def whole(n):
        return sums[chain[2 * sublanes, own + n]]

    def begin(p):
        return core * (cmargin - (p + 1) * csub) + side * p * csub

    def half(o, p, count=csub):
        at = pl.ds(p * csub, count)
        return remote(half_out.at[at], half_in.at[o - 1, at], half_send.at[o - 1], half_recv.at[o - 1, p], peer(o))

    def share(p):
        for n in range(csub):
            half_out[p * csub + n] = whole(begin(p) + n).astype(low)
        for o in range(1, chips):
            half(o, p).start()

    for p in range(early):
        share(p)
    def across(p):
        src = cext.at[pl.ds(cmargin + own + begin(p), csub)]
        return remote(src, clanding.at[pl.ds(begin(p), csub)], cx_send.at[0], cx_recv.at[p], forth)

    def mate(p):
        at = pl.ds(cmargin + own + begin(p), csub)
        return remote(cext.at[at], cext.at[at], mate_sem.at[0], mate_sem.at[1], partner)

    for p in range(parts):
        if p + early < parts:
            share(p + early)
        for o in range(1, chips):
            half(o, p).wait_recv()
        for m in range(csub):
            n = begin(p) + m
            total = whole(n)
            for o in range(1, chips):
                total = total + half_in[o - 1, p * csub + m].astype(f32)
            crhs[n] = total
            value = damping * dot(csmoother[n], total.astype(low))
            cfirst[n] = value
            cext[cmargin + own + n] = value.astype(low)
        pl.when(linked)(lambda: across(p).start())
        mate(p).start()

    cbase = r * cheight - cmargin

    def coarse_residual(n):
        image = row_product(n, coarse_cols, own + n, cbase, cpacked, cext, cmargin + own + n)
        cres[n] = (crhs[n] - image).astype(low)

    def coarse_second(n):
        correction[own + n] = cfirst[n] + damping * dot(csmoother[n], cres[n])

    def back(row):
        at = pl.ds(own + row, chunk)
        return remote(correction.at[at], correction.at[at], cp_sem.at[0], cp_sem.at[1], partner)

    halves = correction.at[mine]
    all_back = remote(halves, halves, cp_sem.at[0], cp_sem.at[1], partner)
    all_mate = remote(clanding, clanding, mate_sem.at[0], mate_sem.at[1], partner)
    all_across = remote(clanding, clanding, cx_send.at[0], cx_recv.at[0], forth)
    all_mate.wait_recv()
    for k in range(parts // group):
        first_row = side * (cmargin - (k + 1) * sublanes) + core * k * sublanes

        def arrived():
            for p in range(k * group, (k + 1) * group):
                across(p).wait_recv()

            def place(n):
                cext[core * (cmargin + cheight) + n] = clanding[n]

            rows(first_row, sublanes, place, 4)

        pl.when(linked)(arrived)
        for n in range(sublanes):
            coarse_residual(first_row + n)
        for quarter in range(0, sublanes, chunk):
            for n in range(chunk):
                coarse_second(first_row + quarter + n)
            back(first_row + quarter).start()
    all_back.wait_recv()

    cstart = r * cheight

    def final(i):
        iterate[i] = iterate[i] + correction[jnp.clip(aggregate[i] - cstart, 0, cheight - 1)]

    rows(0, height, final, 4)

    for n in range(len(drained), len(queue)):
        wait_sent(n)
    name_copy.wait_send()
    near(0, height).wait_send()
    for o in range(1, chips):
        half(o, 0, cmargin).wait_send()

    pl.when(linked)(lambda: all_across.wait_send())
    all_mate.wait_send()
    all_back.wait_send()


def on_device(
    groups, ranks,
    rhs, fine_diag, fine_smoother, fine_blocks, fine_cols, aggregate,
    coarse_diag, coarse_smoother, coarse_blocks, coarse_cols,
):
    height, b, n = rhs.shape
    cheight = coarse_diag.shape[0]
    cmargin = cheight // 2
    neighbours = fine_blocks.shape[1]
    chips = groups // 2
    steps = height // sublanes
    parts = cmargin // csub
    vmem = pltpu.VMEM
    dma = pltpu.SemaphoreType.DMA
    smem = pl.BlockSpec(memory_space=pltpu.SMEM)
    hbm = pl.BlockSpec(memory_space=pl.ANY)
    return pl.pallas_call(
        functools.partial(kernel, groups, ranks),
        out_shape=pltpu.VMEM(rhs.shape, f32),
        in_specs=[smem] * 3 + [hbm] * 7,
        out_specs=pl.BlockSpec(memory_space=pltpu.VMEM),
        scratch_shapes=[
            vmem((height, b, n), f32),
            vmem((height, b, b), low),
            vmem((height, b, b), low),
            vmem((height, neighbours, b, b), low),
            vmem((cmargin, b, b), low),
            vmem((cmargin, b, b), low),
            vmem((cmargin, neighbours, b, b), low),
            vmem((height, b, (neighbours + 1) * b), low),
            vmem((cmargin, b, (neighbours + 1) * b), low),
            vmem((2 * height, b, n), low),
            vmem((2 * height, b, n), low),
            vmem((2, height // 2, b, n), low),
            vmem((2, height // 2, b, n), low),
            vmem((height, b, n), f32),
            vmem((height, b, n), f32),
            vmem((2 * height + 1, b, n), f32),
            vmem((2, sublanes, lanes), jnp.int32),
            vmem((3 * sublanes, lanes), jnp.int32),
            pltpu.SMEM((3 * sublanes, lanes), jnp.int32),
            vmem((cmargin, b, n), low),
            vmem((chips - 1, cmargin, b, n), low),
            vmem((cmargin, b, n), f32),
            vmem((cmargin, b, n), f32),
            vmem((cmargin, b, n), low),
            vmem((2 * cheight, b, n), low),
            vmem((cmargin, b, n), low),
            vmem((cheight, b, n), f32),
            dma((12,)),
            dma((2, depth)),
            dma((2, steps)),
            dma((2,)),
            dma((1,)),
            dma((steps,)),
            dma((chips - 1,)),
            dma((chips - 1, parts)),
            dma((1,)),
            dma((parts,)),
            dma((2,)),
            dma((2,)),
        ],
        compiler_params=pltpu.CompilerParams(
            collective_id=0, has_side_effects=True, vmem_limit_bytes=58 * 1024 * 1024
        ),
        name="cycle",
    )(
        fine_cols.T, coarse_cols.T, aggregate,
        rhs, fine_diag, fine_smoother, fine_blocks, coarse_diag, coarse_smoother, coarse_blocks,
    )


def solution(mesh):
    fine = P(("grp", "rows"))
    return jax.shard_map(
        functools.partial(on_device, mesh.shape["grp"], mesh.shape["rows"]),
        mesh=mesh,
        in_specs=(fine,) * 6 + (P("rows"),) * 4,
        out_specs=fine,
        check_vma=False,
    )
```

```python
import functools

import jax
import jax.numpy as jnp
from jax import lax
from jax.experimental import pallas as pl
from jax.experimental.pallas import tpu as pltpu
from jax.sharding import PartitionSpec as P

MESH = pl.DeviceIdType.MESH
damping = 0.8
lanes = 128
sublanes = 8
depth = 8
fewer = 3
later = 4
early = 8
csub = 2
low = jnp.bfloat16
f32 = jnp.float32


def dot(a, b):
    return jnp.dot(a, b, preferred_element_type=f32)


def pack(i, offs, diag, packed):
    packed[i] = jnp.concatenate([offs[i, k] for k in range(offs.shape[1])] + [diag[i]], axis=1)


def row_product(i, columns, at, base, packed, extended, own):
    count = columns.shape[0]
    width = packed.shape[2] // (count + 1)
    last = extended.shape[0] - 1
    vectors = [extended[jnp.clip(columns[k, at] - base, 0, last)] for k in range(count)] + [extended[own]]
    total = None
    for p in range(0, count + 1, 4):
        group = vectors[p : p + 4]
        term = dot(packed[i, :, width * p : width * (p + len(group))], jnp.concatenate(group, axis=0))
        total = term if total is None else total + term
    return total


def absorb_order(steps):
    order = [(k, t - k) for t in range(steps + 1) for k in (0, 1)]
    return [(k, j) for k, j in order if 0 <= j < steps]


def kernel(
    groups, ranks,
    fine_cols, coarse_cols, aggregate,
    rhs_hbm, diag_hbm, smoother_hbm, blocks_hbm, cdiag_hbm, csmoother_hbm, cblocks_hbm,
    iterate,
    rhs, diag, smoother, blocks, cdiag, csmoother, cblocks, packed, cpacked,
    ext1, ext2, landing1, landing2,
    own_full, near_full, sums, names, tables, chain,
    half_out, half_in, crhs, cfirst, cres, cext, clanding, correction,
    load_sem, halo_send, halo_recv, name_sem, near_send, near_recv,
    half_send, half_recv, cx_send, cx_recv, mate_sem, cp_sem,
):
    g = lax.axis_index("grp")
    r = lax.axis_index("rows")
    height = rhs.shape[0]
    margin = height // 2
    steps = height // sublanes
    chunk = sublanes // 2
    piece = chunk // 2
    cheight = correction.shape[0]
    cmargin = cheight // 2
    chips = groups // 2
    parts = cmargin // csub
    group = sublanes // csub

    flat = g * ranks + r
    has_left = flat > 0
    has_right = flat < groups * ranks - 1
    left = ((flat - 1) // ranks, (flat + ranks - 1) % ranks)
    right = ((flat + 1) // ranks, (flat + 1) % ranks)
    core = g % 2
    chip = g // 2
    partner = (chip * 2 + 1 - core, r)
    side = 1 - core
    forth = (chip * 2 + 1 - core, r - 1 + 2 * core)
    linked = jnp.where(core == 0, r > 0, r < ranks - 1)

    def peer(o):
        return (((chip + o) % chips) * 2 + core, r)

    def load(src, dst, at):
        return pltpu.make_async_copy(src, dst, load_sem.at[at])

    mine = pl.ds(core * cmargin, cmargin)
    edge = sublanes
    pairs = [(rhs_hbm, rhs), (smoother_hbm, smoother)]
    spans = [pl.ds(0, edge), pl.ds(height - edge, edge), pl.ds(edge, height - 2 * edge)]
    edge_loads = [load(a.at[at], b.at[at], 8 + 2 * n + m) for n, at in enumerate(spans[:2]) for m, (a, b) in enumerate(pairs)]
    first_loads = [load(a.at[spans[2]], b.at[spans[2]], m) for m, (a, b) in enumerate(pairs)]
    later_loads = [
        load(blocks_hbm, blocks, 2),
        load(diag_hbm, diag, 3),
        load(csmoother_hbm.at[mine], csmoother, 4),
        load(cdiag_hbm.at[mine], cdiag, 5),
        load(cblocks_hbm.at[mine], cblocks, 6),
    ]
    for c in edge_loads + first_loads:
        c.start()

    barrier = pltpu.get_barrier_semaphore()

    def greet(device):
        pl.semaphore_signal(barrier, inc=1, device_id=device, device_id_type=MESH)

    pl.when(has_left)(lambda: greet(left))
    pl.when(has_right)(lambda: greet(right))
    greet(partner)
    pl.when(linked)(lambda: greet(forth))
    for o in range(1, chips):
        greet(peer(o))
    met = chips + has_left.astype(jnp.int32) + has_right.astype(jnp.int32) + linked.astype(jnp.int32)

    def remote(src, dst, send, recv, device):
        return pltpu.make_async_remote_copy(
            src_ref=src, dst_ref=dst, send_sem=send, recv_sem=recv, device_id=device, device_id_type=MESH
        )

    pieces = margin // piece
    queue = [(0, j * piece, piece) for j in range(pieces)] + [(1, margin - piece, piece)]
    queue += [(1, j * piece, piece) for j in range(pieces - 1)]
    second_queue = pieces + 1
    pushed, drained = [], []
    exts, landings = (ext1, ext2), (landing1, landing2)

    def to_right(n, item=None):
        phase, start, count = item or queue[n]
        src = exts[phase].at[pl.ds(margin + height - start - count, count)]
        dst = landings[phase].at[0, pl.ds(margin - start - count, count)]
        return remote(src, dst, halo_send.at[0, n % depth], halo_recv.at[phase, start // chunk], right)

    def to_left(n, item=None):
        phase, start, count = item or queue[n]
        src = exts[phase].at[pl.ds(margin + start, count)]
        dst = landings[phase].at[1, pl.ds(start, count)]
        return remote(src, dst, halo_send.at[1, n % depth], halo_recv.at[phase, start // chunk], left)

    def wait_sent(n):
        pl.when(has_right)(lambda: to_right(n).wait_send())
        pl.when(has_left)(lambda: to_left(n).wait_send())

    def launch(n):
        if n < second_queue:
            window = depth
        else:
            window = fewer if n < second_queue + 4 else later
        while len(drained) <= n - window:
            wait_sent(len(drained))
            drained.append(None)
        pl.when(has_right)(lambda: to_right(n).start())
        pl.when(has_left)(lambda: to_left(n).start())

    def push(upto):
        while len(pushed) < min(upto, len(queue)):
            launch(len(pushed))
            pushed.append(None)

    def rows(start, count, body, unroll):
        def step(n, carry):
            body(start + n)
            return carry

        lax.fori_loop(0, count, step, 0, unroll=unroll)

    def wait_halo(phase, j):
        start, count = j * chunk, chunk
        ext, landing = exts[phase], landings[phase]
        sides = landing.at[:, pl.ds(start, count)]
        both = remote(sides, sides, halo_send.at[0, 0], halo_recv.at[phase, j], left)
        pl.when(jnp.logical_and(has_left, has_right))(lambda: both.wait_recv())
        pl.when(jnp.logical_not(has_right))(lambda: to_right(0, (phase, start, count)).wait_recv())
        pl.when(jnp.logical_not(has_left))(lambda: to_left(0, (phase, start, count)).wait_recv())

        def place_low(i):
            ext[i] = landing[0, i]

        def place_high(i):
            ext[margin + height + i] = landing[1, i]

        pl.when(has_left)(lambda: rows(margin - start - count, count, place_low, count))
        pl.when(has_right)(lambda: rows(start, count, place_high, count))

    starts = [at for j in range(steps) for at in (margin - (j + 1) * chunk, margin + j * chunk)]

    lane = lax.broadcasted_iota(jnp.int32, (sublanes, lanes), 1)
    sublane = lax.broadcasted_iota(jnp.int32, (sublanes, lanes), 0)
    named = jnp.zeros((sublanes, lanes), jnp.int32)
    for n, start in enumerate(starts):
        for m in range(chunk):
            named = jnp.where(lane == n * chunk + m, aggregate[start + m], named)
    names[0] = named

    name_copy = remote(names.at[0], names.at[1], name_sem.at[0], name_sem.at[1], partner)

    for c in edge_loads:
        c.wait()

    def first(i):
        value = damping * dot(smoother[i], rhs[i].astype(low))
        iterate[i] = value
        ext1[margin + i] = value.astype(low)

    for j in range(steps):
        rows(height - (j + 1) * chunk, chunk, first, 4)
        rows(j * chunk, chunk, first, 4)
        if j == 1:
            pl.semaphore_wait(barrier, met)
            push(2 * j + 2)
            for c in first_loads:
                c.wait()
            for c in later_loads:
                c.start()

        elif 1 < j and 2 * j + 2 <= depth:
            push(2 * j + 2)
    name_copy.start()
    order = absorb_order(steps)
    place_of = {key: 1 + sublanes * n for n, key in enumerate(order)}
    name_copy.wait_recv()
    columns = jnp.zeros((sublanes, lanes), jnp.int32)
    places = []
    for k in (0, 1):
        columns = jnp.where(sublane == k, names[k], columns)
        spot = lane % sublanes
        for j in range(steps):
            spot = jnp.where(lane // sublanes == j, spot + place_of[k, j], spot)
        places.append(spot)
    columns = columns.T
    found = [jnp.zeros((sublanes, lanes), jnp.int32) for _ in range(3)]
    for k in (0, 1):
        for j in range(steps):
            column = jnp.broadcast_to(columns[sublanes * j : sublanes * (j + 1), k : k + 1], (sublanes, lanes))
            spot = place_of[k, j] + sublane
            for i in (0, 1):
                hit = jnp.logical_and(column == names[i], spot < places[i])
                found[i] = jnp.maximum(found[i], jnp.where(hit, spot, 0))
            hit = column == r * cheight + lane
            found[2] = jnp.maximum(found[2], jnp.where(hit, spot, 0))
    for i in range(3):
        best = found[i]
        for shift in (1, 2, 4):
            best = jnp.maximum(best, pltpu.roll(best, shift, 0))
        tables[pl.ds(sublanes * i, sublanes)] = best
    to_scalar = load(tables, chain, 7)
    to_scalar.start()
    sums[0] = jnp.zeros(sums.shape[1:], f32)
    to_scalar.wait()
    later_loads[0].wait()
    later_loads[1].wait()

    base = flat * height - margin

    def residual_low(i):
        residual = rhs[i] - row_product(i, fine_cols, i, base, packed, ext1, margin + i)
        ext2[margin + i] = residual.astype(low)

    def second(i):
        value = iterate[i] + damping * dot(smoother[i], ext2[margin + i])
        iterate[i] = value
        ext2[margin + i] = value.astype(low)

    def pack_step(j):
        for start in starts[2 * j : 2 * j + 2]:
            rows(start, chunk, lambda i: pack(i, blocks, diag, packed), 2)

    pack_step(0)
    pack_step(1)
    for j in range(steps):
        push(min(2 * j + 2 + depth, second_queue))
        if j + 2 < steps:
            pack_step(j + 2)
        if j == 1:
            for c in later_loads[2:]:
                c.wait()
        if 1 <= j < 5:
            share_rows = cmargin // 4
            rows((j - 1) * share_rows, share_rows, lambda i: pack(i, cblocks, cdiag, cpacked), 2)
        wait_halo(0, j)
        picks = [starts[2 * j + n // chunk] + n % chunk for n in range(sublanes)]
        if j == steps - 1:
            picks.sort(key=lambda i: min(i, height - 1 - i))
        for batch in [picks] if j < steps - 1 else [picks[: 2 * piece], picks[2 * piece :]]:
            for body in (residual_low, second):
                for i in batch:
                    body(i)
            if j == steps - 1:
                push(len(pushed) + 1)

    def third(i, at):
        residual = rhs[i] - row_product(i, fine_cols, i, base, packed, ext2, margin + i)
        own_full[at] = residual

    def near(j, count=sublanes):
        at = pl.ds(j * sublanes, count)
        return remote(own_full.at[at], near_full.at[at], near_send.at[0], near_recv.at[j], partner)

    def absorb(k, j):
        source = (own_full, near_full)[k]
        spot = place_of[k, j] - j * sublanes

        def body(at):
            sums[at + spot] = source[at] + sums[chain[sublanes * k, at]]

        rows(j * sublanes, sublanes, body, 4)

    for k, j in order:
        if k == 0:
            push(second_queue + 2 * j + 2 + later)
            wait_halo(1, j)
            for n in range(sublanes):
                third(starts[2 * j + n // chunk] + n % chunk, j * sublanes + n)
            near(j).start()
        else:
            near(j).wait_recv()
        absorb(k, j)

    own = core * cmargin

    def whole(n):
        return sums[chain[2 * sublanes, own + n]]

    def begin(p):
        return core * (cmargin - (p + 1) * csub) + side * p * csub

    def half(o, p, count=csub):
        at = pl.ds(p * csub, count)
        return remote(half_out.at[at], half_in.at[o - 1, at], half_send.at[o - 1], half_recv.at[o - 1, p], peer(o))

    def share(p):
        for n in range(csub):
            half_out[p * csub + n] = whole(begin(p) + n).astype(low)
        for o in range(1, chips):
            half(o, p).start()

    for p in range(early):
        share(p)
    def across(p):
        src = cext.at[pl.ds(cmargin + own + begin(p), csub)]
        return remote(src, clanding.at[pl.ds(begin(p), csub)], cx_send.at[0], cx_recv.at[p], forth)

    def mate(p):
        at = pl.ds(cmargin + own + begin(p), csub)
        return remote(cext.at[at], cext.at[at], mate_sem.at[0], mate_sem.at[1], partner)

    for p in range(parts):
        if p + early < parts:
            share(p + early)
        for o in range(1, chips):
            half(o, p).wait_recv()
        for m in range(csub):
            n = begin(p) + m
            total = whole(n)
            for o in range(1, chips):
                total = total + half_in[o - 1, p * csub + m].astype(f32)
            crhs[n] = total
            value = damping * dot(csmoother[n], total.astype(low))
            cfirst[n] = value
            cext[cmargin + own + n] = value.astype(low)
        pl.when(linked)(lambda: across(p).start())
        mate(p).start()

    cbase = r * cheight - cmargin

    def coarse_residual(n):
        image = row_product(n, coarse_cols, own + n, cbase, cpacked, cext, cmargin + own + n)
        cres[n] = (crhs[n] - image).astype(low)

    def coarse_second(n):
        correction[own + n] = cfirst[n] + damping * dot(csmoother[n], cres[n])

    def back(row):
        at = pl.ds(own + row, chunk)
        return remote(correction.at[at], correction.at[at], cp_sem.at[0], cp_sem.at[1], partner)

    halves = correction.at[mine]
    all_back = remote(halves, halves, cp_sem.at[0], cp_sem.at[1], partner)
    all_mate = remote(clanding, clanding, mate_sem.at[0], mate_sem.at[1], partner)
    all_across = remote(clanding, clanding, cx_send.at[0], cx_recv.at[0], forth)
    all_mate.wait_recv()
    for k in range(parts // group):
        first_row = side * (cmargin - (k + 1) * sublanes) + core * k * sublanes

        def arrived():
            for p in range(k * group, (k + 1) * group):
                across(p).wait_recv()

            def place(n):
                cext[core * (cmargin + cheight) + n] = clanding[n]

            rows(first_row, sublanes, place, 4)

        pl.when(linked)(arrived)
        for n in range(sublanes):
            coarse_residual(first_row + n)
        for quarter in range(0, sublanes, chunk):
            for n in range(chunk):
                coarse_second(first_row + quarter + n)
            back(first_row + quarter).start()
    all_back.wait_recv()

    cstart = r * cheight

    def final(i):
        iterate[i] = iterate[i] + correction[jnp.clip(aggregate[i] - cstart, 0, cheight - 1)]

    rows(0, height, final, 4)

    for n in range(len(drained), len(queue)):
        wait_sent(n)
    name_copy.wait_send()
    near(0, height).wait_send()
    for o in range(1, chips):
        half(o, 0, cmargin).wait_send()

    pl.when(linked)(lambda: all_across.wait_send())
    all_mate.wait_send()
    all_back.wait_send()


def on_device(
    groups, ranks,
    rhs, fine_diag, fine_smoother, fine_blocks, fine_cols, aggregate,
    coarse_diag, coarse_smoother, coarse_blocks, coarse_cols,
):
    height, b, n = rhs.shape
    cheight = coarse_diag.shape[0]
    cmargin = cheight // 2
    neighbours = fine_blocks.shape[1]
    chips = groups // 2
    steps = height // sublanes
    parts = cmargin // csub
    vmem = pltpu.VMEM
    dma = pltpu.SemaphoreType.DMA
    smem = pl.BlockSpec(memory_space=pltpu.SMEM)
    hbm = pl.BlockSpec(memory_space=pl.ANY)
    return pl.pallas_call(
        functools.partial(kernel, groups, ranks),
        out_shape=pltpu.VMEM(rhs.shape, f32),
        in_specs=[smem] * 3 + [hbm] * 7,
        out_specs=pl.BlockSpec(memory_space=pltpu.VMEM),
        scratch_shapes=[
            vmem((height, b, n), f32),
            vmem((height, b, b), low),
            vmem((height, b, b), low),
            vmem((height, neighbours, b, b), low),
            vmem((cmargin, b, b), low),
            vmem((cmargin, b, b), low),
            vmem((cmargin, neighbours, b, b), low),
            vmem((height, b, (neighbours + 1) * b), low),
            vmem((cmargin, b, (neighbours + 1) * b), low),
            vmem((2 * height, b, n), low),
            vmem((2 * height, b, n), low),
            vmem((2, height // 2, b, n), low),
            vmem((2, height // 2, b, n), low),
            vmem((height, b, n), f32),
            vmem((height, b, n), f32),
            vmem((2 * height + 1, b, n), f32),
            vmem((2, sublanes, lanes), jnp.int32),
            vmem((3 * sublanes, lanes), jnp.int32),
            pltpu.SMEM((3 * sublanes, lanes), jnp.int32),
            vmem((cmargin, b, n), low),
            vmem((chips - 1, cmargin, b, n), low),
            vmem((cmargin, b, n), f32),
            vmem((cmargin, b, n), f32),
            vmem((cmargin, b, n), low),
            vmem((2 * cheight, b, n), low),
            vmem((cmargin, b, n), low),
            vmem((cheight, b, n), f32),
            dma((12,)),
            dma((2, depth)),
            dma((2, steps)),
            dma((2,)),
            dma((1,)),
            dma((steps,)),
            dma((chips - 1,)),
            dma((chips - 1, parts)),
            dma((1,)),
            dma((parts,)),
            dma((2,)),
            dma((2,)),
        ],
        compiler_params=pltpu.CompilerParams(
            collective_id=0, has_side_effects=True, vmem_limit_bytes=58 * 1024 * 1024
        ),
        name="cycle",
    )(
        fine_cols.T, coarse_cols.T, aggregate,
        rhs, fine_diag, fine_smoother, fine_blocks, coarse_diag, coarse_smoother, coarse_blocks,
    )


def solution(mesh):
    fine = P(("grp", "rows"))
    return jax.shard_map(
        functools.partial(on_device, mesh.shape["grp"], mesh.shape["rows"]),
        mesh=mesh,
        in_specs=(fine,) * 6 + (P("rows"),) * 4,
        out_specs=fine,
        check_vma=False,
    )
```
